512 devices in a mesh: row: 16 (over y, core), col: 32 (over z, x).
Axes of the slice: x: 4, y: 8, z: 8, core: 2. Of those that a mesh axis runs over, the one named last changes fastest.
Arguments:
- matrix: float32 [16384, 16384], P('row', 'col'), as said below
Outputs:
- hess_panel: float32 [16384, 8], P('row')
- reflectors: float32 [16384, 8], P('row')
- wy_products: float32 [16384, 8], P('row')
- wy_factor: float32 [8, 8], replicated
Inputs may be any that keep to these rules, and one draw needn't show every extreme that they name: Entries matrix[i+1, i] lie within 2.5 +- 6 / sqrt(16384); every other entry within +- 6 / sqrt(16384).
All inputs are finite; a program needn't handle non-finite values.
Results may differ from the reference program's by a relative error of at most 0.0003.
Values sent between devices are 32-bit elements; how exact they have to be, the bound alone decides.
A program may use at most 128 MiB of HBM per device.

```python
import math
import jax
import jax.numpy as jnp
from jax import lax

N = 16384
NB = 8


def draw_matrix(key, part):
    first = jax.random.fold_in(key, 11)
    base = jax.random.truncated_normal(first, -6.0, 6.0, (N, N), jnp.float32)
    return base / math.sqrt(N) + 2.5 * jnp.eye(N, k=-1, dtype=jnp.float32)


def setup_inputs(seed: int = 0) -> dict:
    key_of = jax.random.split(jax.random.key(seed), 2)
    matrix = draw_matrix(jax.random.fold_in(key_of[1], 71), 0)
    return {"matrix": matrix}


def reference(matrix):
    exact = lax.Precision.HIGHEST
    order = matrix.shape[0]
    row_ids = jnp.arange(order, dtype=jnp.int32)
    refl = jnp.zeros((order, NB), jnp.float32)
    wy_prod = jnp.zeros((order, NB), jnp.float32)
    factor = jnp.zeros((NB, NB), jnp.float32)
    columns = []
    for column in range(NB):
        current = matrix[:, column] - jnp.dot(wy_prod, refl[column], precision=exact)
        inner = jnp.dot(current, refl, precision=exact)
        current = current - jnp.dot(refl, jnp.dot(inner, factor, precision=exact), precision=exact)
        masked = jnp.where(row_ids > column, current, jnp.float32(0.0))
        leading = current[column + 1]
        length = jnp.sqrt(jnp.sum(masked * masked))
        orient = jnp.where(leading >= 0, jnp.float32(1.0), jnp.float32(-1.0))
        pivot_value = -orient * length
        vector = masked + jnp.where(row_ids == column + 1, orient * length, jnp.float32(0.0))
        vector = vector / jnp.sqrt(length * (length + jnp.abs(leading)))
        coupling = jnp.dot(vector, refl, precision=exact)
        image = jnp.dot(matrix, vector, precision=exact)
        new_y = image - jnp.dot(wy_prod, coupling, precision=exact)
        new_t = -jnp.dot(factor, coupling, precision=exact)
        factor = factor.at[:, column].set(new_t).at[column, column].set(jnp.float32(1.0))
        wy_prod = wy_prod.at[:, column].set(new_y)
        refl = refl.at[:, column].set(vector)
        columns.append(jnp.where(row_ids <= column, current, jnp.where(row_ids == column + 1, pivot_value, jnp.float32(0.0))))
    return (jnp.stack(columns, axis=1), refl, wy_prod, factor)
```

```python
import functools

import jax
import jax.numpy as jnp
from jax import lax
from jax.experimental import pallas as pl
from jax.experimental.pallas import tpu as pltpu
from jax.sharding import PartitionSpec as P

NB = 8
LANES = 128
SUB = 8
STATS = 16
BLOCK = 256
F32 = jnp.float32
BF16 = jnp.bfloat16


def kernel(
    nrow, ncol, a_hbm, hess_ref, refl_ref, wy_ref, fac_ref,
    a_ref, first_ref, pan_ref, mypan_ref, part_ref, got_ref, stat_ref, stats_ref,
    vec_ref, yvec_ref,
    load_sem, first_sem, pan_send, pan_sem, stat_send, stat_sem,
    part_send, part_sem, v_send, v_sem, y_send, y_sem,
):
    rows_local, cols_local = a_hbm.shape
    tiles = cols_local // LANES
    lines = rows_local // LANES
    split = rows_local // cols_local
    row, col = lax.axis_index("row"), lax.axis_index("col")
    blocks = rows_local // BLOCK
    owner = col // split
    slot = col - owner * split
    home = owner == row
    last = NB - 1

    def wrap(value, bound):
        return jnp.where(value >= bound, value - bound, value)

    def far_first(count):
        return sorted(range(count), key=lambda d: -min(d, count - d))

    def block_load(i):
        span = pl.ds(i * BLOCK, BLOCK)
        return pltpu.make_async_copy(a_hbm.at[span], a_ref.at[span], load_sem.at[i])

    head = pltpu.make_async_copy(a_hbm.at[:, pl.ds(0, LANES)], first_ref, first_sem)

    @pl.when(col == 0)
    def _():
        head.start()

    for i in range(blocks):
        block_load(i).start(priority=1)

    barrier = pltpu.get_barrier_semaphore()

    def greet(to_row, to_col):
        pl.semaphore_signal(
            barrier, inc=1, device_id=(to_row, to_col),
            device_id_type=pl.DeviceIdType.MESH,
        )

    for dc in far_first(ncol)[:-1]:
        greet(owner, wrap(col + dc, ncol))

    @pl.when(jnp.logical_not(home))
    def _():
        greet(owner, col)

    for dc in far_first(ncol)[:-1]:
        greet(row, wrap(col + dc, ncol))

    def send(src, dst, send_sem, recv_sem, to_row, to_col):
        pltpu.make_async_remote_copy(
            src_ref=src, dst_ref=dst, send_sem=send_sem, recv_sem=recv_sem,
            device_id=(to_row, to_col), device_id_type=pl.DeviceIdType.MESH,
        ).start()

    def place(src, dst, send_sem, recv_sem, to_row, to_col, here):
        @pl.when(here)
        def _():
            pltpu.make_async_copy(src, dst, recv_sem).start()

        @pl.when(jnp.logical_not(here))
        def _():
            send(src, dst, send_sem, recv_sem, to_row, to_col)

    def to_peers(src, dst, send_sem, recv_sem):
        for dc in far_first(ncol)[:-1]:
            send(src, dst, send_sem, recv_sem, row, wrap(col + dc, ncol))

    def expect(ref, sem):
        pltpu.make_async_copy(ref, ref, sem).wait()

    def settle(ref, sem, here):
        count = ref.shape[1]

        @pl.when(jnp.logical_not(here))
        def _():
            expect(ref, sem)

        if count > 1:
            @pl.when(here)
            def _():
                expect(ref.at[:, pl.ds(0, count - 1)], sem)

    def spread(h, src, dst, send_sem, recv_sem):
        to_col = row * split + h
        for dr in far_first(nrow)[:-1]:
            send(src, dst, send_sem, recv_sem, wrap(row + dr, nrow), to_col)
        place(src, dst, send_sem, recv_sem, row, to_col, to_col == col)

    @pl.when(col == 0)
    def _():
        head.wait()
        for h in range(split):
            def turn(t, carry):
                at = pl.multiple_of(h * cols_local + t * LANES, LANES)
                block = first_ref[pl.ds(at, LANES), :].T
                for k in range(NB + 1):
                    pan_ref[k, h, pl.ds(t, 1), :] = block[k : k + 1, :]
                return carry

            lax.fori_loop(0, tiles, turn, 0)

    partners = split * nrow + ncol - 1
    pl.semaphore_wait(barrier, jnp.where(home, partners - 1, partners))

    def pan_span(i):
        return pl.ds(0, 1) if i == 0 else pl.ds(2 * i - 1, 2)

    def send_pan(i):
        @pl.when(col == 0)
        def _():
            for h in range(split):
                spread(
                    h, pan_ref.at[pan_span(i), h], mypan_ref.at[pan_span(i)],
                    pan_send, pan_sem.at[i],
                )

    send_pan(0)
    send_pan(1)

    ones = jnp.ones((SUB, 2 * LANES), BF16)

    def fold(acc, h, t, j):
        high = acc.astype(BF16)
        low = (acc - high.astype(F32)).astype(BF16)
        both = jnp.concatenate([high, low], axis=1)
        res = lax.dot_general(
            ones, both, (((1,), (1,)), ((), ())), preferred_element_type=F32
        )
        part_ref[j, h, pl.ds(t, 1), :] = res[0:1, :]

    def matvec(j, vector, act):
        pieces = [
            jnp.broadcast_to(vector[t : t + 1, :], (SUB, LANES)) for t in range(tiles)
        ]

        def product(t):
            accs = []
            for s in range(LANES // SUB):
                at = pl.ds(pl.multiple_of(t * LANES + s * SUB, SUB), SUB)
                acc = a_ref[at, pl.ds(0, LANES)] * pieces[0]
                for p in range(1, tiles):
                    acc = acc + a_ref[at, pl.ds(p * LANES, LANES)] * pieces[p]
                accs.append(acc)
            return jnp.concatenate(accs, axis=0)

        for h in range(split):
            def step(t, acc):
                fold(acc, h, t - 1, j)
                return product(h * tiles + t)

            fold(lax.fori_loop(1, tiles, step, product(h * tiles)), h, tiles - 1, j)
            act(h)

    def publish(src, ref, j, send_sem, recv_sem):
        for i in range(split):
            to_col = row * split + i
            here = jnp.logical_and(home, to_col == col)
            place(src, ref.at[j, slot], send_sem, recv_sem, owner, to_col, here)

    lane = lax.broadcasted_iota(jnp.int32, (1, LANES), 1)
    at_stat = lax.broadcasted_iota(jnp.int32, (STATS, LANES), 0) + STATS
    at_lane = lax.broadcasted_iota(jnp.int32, (STATS, LANES), 1)
    line_ids = lax.broadcasted_iota(jnp.int32, (tiles, LANES), 0) * LANES
    ids = line_ids + lax.broadcasted_iota(jnp.int32, (tiles, LANES), 1)
    ids = ids + col * cols_local
    hess_ref[...] = jnp.zeros_like(hess_ref)

    def send_stats(j, b):
        rows = [jnp.sum(vec_ref[k] * b, axis=0, keepdims=True) for k in range(j)]
        rows += [jnp.zeros((1, LANES), F32)] * (NB - j)
        rows.append(jnp.sum(b * b, axis=0, keepdims=True))
        rows += [jnp.zeros((1, LANES), F32)] * (STATS - NB - 1)
        sums = jnp.sum(jnp.concatenate(rows, axis=0), axis=1, keepdims=True)
        packed = jnp.where(at_lane == at_stat, sums, F32(0.0))
        packed = jnp.sum(packed, axis=0, keepdims=True)
        top = jnp.where(jnp.logical_and(col == 0, lane < STATS), b[0:1, :], packed)
        stat_ref[j] = top
        stats_ref[j, col] = top
        to_peers(stat_ref.at[j], stats_ref.at[j, col], stat_send, stat_sem.at[j])

    def total(ref, j, count):
        terms = [ref[j, i] for i in range(count)]
        while len(terms) > 1:
            terms = [x + y for x, y in zip(terms[::2], terms[1::2])]
        return terms[0]

    factor = [[None] * NB for _ in range(NB)]
    gram = [[None] * NB for _ in range(NB)]
    tops = []
    images = []
    for i in range(blocks):
        block_load(i).wait()
    expect(mypan_ref.at[pan_span(0)], pan_sem.at[0])
    b = mypan_ref[0]
    for j in range(NB):
        if j < last:
            matvec(j, b, lambda h: spread(
                h, part_ref.at[j, h], got_ref.at[j, col], part_send, part_sem.at[j]
            ))
            send_stats(j, b)
            if j > 0:
                publish(vec_ref.at[j - 1], refl_ref, j - 1, v_send, v_sem)
                publish(yvec_ref.at[j - 1], wy_ref, j - 1, y_send, y_sem)
            if 0 < j < NB // 2:
                send_pan(j + 1)
        else:
            send_stats(j, b)

            def to_owner(h):
                to_col = row * split + h
                place(
                    part_ref.at[j, h], got_ref.at[j, col], part_send, part_sem.at[j],
                    row, to_col, to_col == col,
                )

            matvec(j, b, to_owner)
            publish(vec_ref.at[j - 1], refl_ref, j - 1, v_send, v_sem)
            publish(yvec_ref.at[j - 1], wy_ref, j - 1, y_send, y_sem)

        expect(stats_ref.at[j, pl.ds(0, ncol - 1)], stat_sem.at[j])
        stat = total(stats_ref, j, ncol)
        inner = [stat[:, STATS + k : STATS + k + 1] for k in range(j)]
        top = jnp.where(lane < STATS, stat, F32(0.0))
        weight = []
        for m in range(j):
            value = factor[0][m] * inner[0]
            for k in range(1, m + 1):
                value = value + factor[k][m] * inner[k]
            weight.append(value)
        for m in range(j):
            top = top - tops[m] * weight[m]
        above = jnp.where(lane <= j, top, F32(0.0))
        square = stat[:, STATS + NB : STATS + NB + 1]
        square = square - jnp.sum(above * above, axis=1, keepdims=True)
        norm = jnp.sqrt(square)
        alpha = top[:, j + 1 : j + 2]
        signed = jnp.where(alpha >= 0, norm, -norm)
        scale = 1.0 / jnp.sqrt(norm * (norm + jnp.abs(alpha)))
        u = b
        for m in range(j):
            u = u - vec_ref[m] * weight[m]
        u = jnp.where(ids > j, u, F32(0.0)) + jnp.where(ids == j + 1, signed, F32(0.0))
        u = u * scale
        vec_ref[j] = u
        if j == last:
            @pl.when(home)
            def _():
                to_peers(vec_ref.at[j], refl_ref.at[j, slot], v_send, v_sem)
                pltpu.make_async_copy(vec_ref.at[j], refl_ref.at[j, slot], v_sem).start()
        vtop = jnp.where(lane > j, top, F32(0.0))
        vtop = (vtop + jnp.where(lane == j + 1, signed, F32(0.0))) * scale
        couple = []
        for k in range(j):
            value = inner[k]
            for m in range(j):
                value = value - gram[k][m] * weight[m]
            fix = jnp.where(lane == j + 1, signed, F32(0.0)) - above
            value = value + jnp.sum(tops[k] * fix, axis=1, keepdims=True)
            couple.append(value * scale)
        for k in range(j):
            value = factor[k][k] * couple[k]
            for m in range(k + 1, j):
                value = value + factor[k][m] * couple[m]
            factor[k][j] = -value
            gram[k][j] = couple[k]
            gram[j][k] = couple[k]
        factor[j][j] = jnp.ones((1, 1), F32)
        gram[j][j] = jnp.full((1, 1), 2.0, F32)
        tops.append(vtop)
        hrow = jnp.where(lane == j + 1, -signed, above)
        hess_ref[j, 0, 0:1, :] = jnp.where(row == 0, hrow, F32(0.0))
        if j % 2 == 0:
            expect(mypan_ref.at[pan_span(j // 2 + 1)], pan_sem.at[j // 2 + 1])
        drop = jnp.zeros((tiles, LANES), F32)
        for k in range(j):
            drop = drop + images[k] * weight[k]
        for i in range(j + 1):
            drop = drop + mypan_ref[i] * top[:, i : i + 1]
        drop = (drop - mypan_ref[j + 1] * signed) * scale
        back = jnp.zeros((tiles, LANES), F32)
        for k in range(j):
            back = back + yvec_ref[k] * couple[k]
        if j < last:
            rest = mypan_ref[j + 1]
            for k in range(j):
                rest = rest - yvec_ref[k] * tops[k][:, j + 1 : j + 2]
            pull = vtop[:, j + 1 : j + 2]
            rest = rest + (drop + back) * pull
            pull = pull * scale

            expect(got_ref.at[j], part_sem.at[j])
            image = total(got_ref, j, ncol)
            b = rest - image * pull
            image = image * scale - drop
            images.append(image)
            yvec_ref[j] = image - back
        else:
            @pl.when(home)
            def _():
                expect(got_ref.at[j], part_sem.at[j])
                image = total(got_ref, j, ncol)
                yvec_ref[j] = image * scale - drop - back
                to_peers(yvec_ref.at[j], wy_ref.at[j, slot], y_send, y_sem)
                pltpu.make_async_copy(yvec_ref.at[j], wy_ref.at[j, slot], y_sem).start()

    at_row = lax.broadcasted_iota(jnp.int32, (NB, NB), 0)
    at_col = lax.broadcasted_iota(jnp.int32, (NB, NB), 1)
    fac = jnp.zeros((NB, NB), F32)
    for k in range(NB):
        for m in range(k, NB):
            here = jnp.logical_and(at_row == k, at_col == m)
            fac = jnp.where(here, jnp.broadcast_to(factor[k][m], (NB, NB)), fac)
    fac_ref[...] = fac

    expect(stats_ref.at[:, pl.ds(0, ncol - 1)], stat_send)
    settle(got_ref.at[pl.ds(0, last)], part_send, home)
    settle(got_ref.at[pl.ds(0, 1), pl.ds(0, split)], part_send, home)
    settle(refl_ref.at[pl.ds(0, last)], v_send, home)
    settle(wy_ref.at[pl.ds(0, last)], y_send, home)

    @pl.when(home)
    def _():
        expect(got_ref.at[0, pl.ds(0, ncol - 1)], v_send)
        expect(got_ref.at[0, pl.ds(0, ncol - 1)], y_send)

    @pl.when(col == 0)
    def _():
        settle(got_ref.at[pl.ds(0, 1)], pan_send, row == 0)
        settle(got_ref, pan_send, row == 0)

    expect(refl_ref, v_sem)
    expect(wy_ref, y_sem)


def finish(hess_in, refl_in, wy_in, fac_in, hess_out, refl_out, wy_out, fac_out):
    split, tiles = hess_in.shape[1:3]
    for src, dst in ((hess_in, hess_out), (refl_in, refl_out), (wy_in, wy_out)):
        for h in range(split):
            for t in range(tiles):
                span = pl.ds((h * tiles + t) * LANES, LANES)
                for k in range(NB):
                    dst[k : k + 1, span] = src[k, h, t : t + 1, :]
    fac_out[...] = fac_in[...]


def shards(nrow, ncol, matrix):
    rows_local, cols_local = matrix.shape
    tiles = cols_local // LANES
    split = rows_local // cols_local
    blocks = rows_local // BLOCK
    panel = jax.ShapeDtypeStruct((NB, split, tiles, LANES), F32)
    vmem = pl.BlockSpec(memory_space=pltpu.VMEM)
    dma = pltpu.SemaphoreType.DMA
    hess, refl, wy, fac = pl.pallas_call(
        functools.partial(kernel, nrow, ncol),
        out_shape=(panel, panel, panel, jax.ShapeDtypeStruct((NB, NB), F32)),
        in_specs=[pl.BlockSpec(memory_space=pl.ANY)],
        out_specs=(vmem, vmem, vmem, vmem),
        scratch_shapes=[
            pltpu.VMEM((rows_local, cols_local), F32),
            pltpu.VMEM((rows_local, LANES), F32),
            pltpu.VMEM((NB + 1, split, tiles, LANES), F32),
            pltpu.VMEM((NB + 1, tiles, LANES), F32),
            pltpu.VMEM((NB, split, tiles, LANES), F32),
            pltpu.VMEM((NB, ncol, tiles, LANES), F32),
            pltpu.VMEM((NB, 1, LANES), F32),
            pltpu.VMEM((NB, ncol, 1, LANES), F32),
            pltpu.VMEM((NB, tiles, LANES), F32),
            pltpu.VMEM((NB, tiles, LANES), F32),
            dma((blocks,)),
            dma(()),
            dma(()),
            dma((NB // 2 + 1,)),
            dma(()),
            dma((NB,)),
            dma(()),
            dma((NB,)),
            dma(()),
            dma(()),
            dma(()),
            dma(()),
        ],
        compiler_params=pltpu.CompilerParams(
            collective_id=0, has_side_effects=True, vmem_limit_bytes=56 * 2**20
        ),
    )(matrix)

    flat = jax.ShapeDtypeStruct((NB, rows_local), F32)
    hess, refl, wy, fac = pl.pallas_call(
        finish,
        out_shape=(flat, flat, flat, jax.ShapeDtypeStruct((NB, NB), F32)),
        in_specs=[vmem] * 4,
        out_specs=(vmem,) * 4,
    )(hess, refl, wy, fac)
    return hess.T, refl.T, wy.T, fac


def solution(mesh):
    nrow, ncol = mesh.shape["row"], mesh.shape["col"]
    return jax.shard_map(
        functools.partial(shards, nrow, ncol),
        mesh=mesh,
        in_specs=(P("row", "col"),),
        out_specs=(P("row", None), P("row", None), P("row", None), P()),
        check_vma=False,
    )
```

```python
import functools

import jax
import jax.numpy as jnp
from jax import lax
from jax.experimental import pallas as pl
from jax.experimental.pallas import tpu as pltpu
from jax.sharding import PartitionSpec as P

NB = 8
LANES = 128
SUB = 8
STATS = 16
BLOCK = 256
F32 = jnp.float32
BF16 = jnp.bfloat16


def kernel(
    nrow, ncol, a_hbm, hess_ref, refl_ref, wy_ref, fac_ref,
    a_ref, first_ref, pan_ref, mypan_ref, part_ref, got_ref, stat_ref, stats_ref,
    vec_ref, yvec_ref, edges_ref, tail_ref, ends_ref, sums_ref,
    load_sem, first_sem, pan_send, pan_sem, stat_send, stat_sem,
    part_send, part_sem, v_send, v_sem, y_send, y_sem,
    edge_send, edge_sem, tail_send, tail_sem, sum_send, sum_sem,
):
    rows_local, cols_local = a_hbm.shape
    tiles = cols_local // LANES
    lines = rows_local // LANES
    split = rows_local // cols_local
    row, col = lax.axis_index("row"), lax.axis_index("col")
    blocks = rows_local // BLOCK
    owner = col // split
    slot = col - owner * split
    home = owner == row
    last = NB - 1

    def wrap(value, bound):
        return jnp.where(value >= bound, value - bound, value)

    def far_first(count):
        return sorted(range(count), key=lambda d: -min(d, count - d))

    def block_load(i):
        span = pl.ds(i * BLOCK, BLOCK)
        return pltpu.make_async_copy(a_hbm.at[span], a_ref.at[span], load_sem.at[i])

    head = pltpu.make_async_copy(a_hbm.at[:, pl.ds(0, LANES)], first_ref, first_sem)

    @pl.when(col == 0)
    def _():
        head.start()

    for i in range(blocks):
        block_load(i).start(priority=1)

    barrier = pltpu.get_barrier_semaphore()

    def greet(to_row, to_col):
        pl.semaphore_signal(
            barrier, inc=1, device_id=(to_row, to_col),
            device_id_type=pl.DeviceIdType.MESH,
        )

    for dc in far_first(ncol)[:-1]:
        greet(owner, wrap(col + dc, ncol))

    @pl.when(jnp.logical_not(home))
    def _():
        greet(owner, col)

    for dc in far_first(ncol)[:-1]:
        greet(row, wrap(col + dc, ncol))

    def send(src, dst, send_sem, recv_sem, to_row, to_col):
        pltpu.make_async_remote_copy(
            src_ref=src, dst_ref=dst, send_sem=send_sem, recv_sem=recv_sem,
            device_id=(to_row, to_col), device_id_type=pl.DeviceIdType.MESH,
        ).start()

    def place(src, dst, send_sem, recv_sem, to_row, to_col, here):
        @pl.when(here)
        def _():
            pltpu.make_async_copy(src, dst, recv_sem).start()

        @pl.when(jnp.logical_not(here))
        def _():
            send(src, dst, send_sem, recv_sem, to_row, to_col)

    def to_peers(src, dst, send_sem, recv_sem):
        for dc in far_first(ncol)[:-1]:
            send(src, dst, send_sem, recv_sem, row, wrap(col + dc, ncol))

    def expect(ref, sem):
        pltpu.make_async_copy(ref, ref, sem).wait()

    def settle(ref, sem, here):
        count = ref.shape[1]

        @pl.when(jnp.logical_not(here))
        def _():
            expect(ref, sem)

        if count > 1:
            @pl.when(here)
            def _():
                expect(ref.at[:, pl.ds(0, count - 1)], sem)

    def spread(h, src, dst, send_sem, recv_sem):
        to_col = row * split + h
        for dr in far_first(nrow)[:-1]:
            send(src, dst, send_sem, recv_sem, wrap(row + dr, nrow), to_col)
        place(src, dst, send_sem, recv_sem, row, to_col, to_col == col)

    @pl.when(col == 0)
    def _():
        head.wait()
        for h in range(split):
            def turn(t, carry):
                at = pl.multiple_of(h * cols_local + t * LANES, LANES)
                block = first_ref[pl.ds(at, LANES), :].T
                for k in range(NB + 1):
                    pan_ref[k, h, pl.ds(t, 1), :] = block[k : k + 1, :]
                return carry

            lax.fori_loop(0, tiles, turn, 0)

    partners = split * nrow + ncol - 1
    pl.semaphore_wait(barrier, jnp.where(home, partners - 1, partners))

    def pan_span(i):
        return pl.ds(0, 1) if i == 0 else pl.ds(2 * i - 1, 2)

    def send_pan(i):
        @pl.when(col == 0)
        def _():
            for h in range(split):
                spread(
                    h, pan_ref.at[pan_span(i), h], mypan_ref.at[pan_span(i)],
                    pan_send, pan_sem.at[i],
                )

    send_pan(0)
    send_pan(1)

    ones = jnp.ones((SUB, 2 * LANES), BF16)

    def fold(acc, h, t, j):
        high = acc.astype(BF16)
        low = (acc - high.astype(F32)).astype(BF16)
        both = jnp.concatenate([high, low], axis=1)
        res = lax.dot_general(
            ones, both, (((1,), (1,)), ((), ())), preferred_element_type=F32
        )
        part_ref[j, h, pl.ds(t, 1), :] = res[0:1, :]

    def matvec(j, vector, act):
        pieces = [
            jnp.broadcast_to(vector[t : t + 1, :], (SUB, LANES)) for t in range(tiles)
        ]

        def product(t):
            accs = []
            for s in range(LANES // SUB):
                at = pl.ds(pl.multiple_of(t * LANES + s * SUB, SUB), SUB)
                acc = a_ref[at, pl.ds(0, LANES)] * pieces[0]
                for p in range(1, tiles):
                    acc = acc + a_ref[at, pl.ds(p * LANES, LANES)] * pieces[p]
                accs.append(acc)
            return jnp.concatenate(accs, axis=0)

        for h in range(split):
            def step(t, acc):
                fold(acc, h, t - 1, j)
                return product(h * tiles + t)

            fold(lax.fori_loop(1, tiles, step, product(h * tiles)), h, tiles - 1, j)
            act(h)

    def own_rows(src, dst, send_sem, recv_sem):
        @pl.when(home)
        def _():
            to_peers(src, dst(slot), send_sem, recv_sem)
            pltpu.make_async_copy(src, dst(slot), recv_sem).start()

    def publish(src, ref, j, send_sem, recv_sem):
        for i in range(split):
            to_col = row * split + i
            here = jnp.logical_and(home, to_col == col)
            place(src, ref.at[j, slot], send_sem, recv_sem, owner, to_col, here)

    lane = lax.broadcasted_iota(jnp.int32, (1, LANES), 1)
    at_stat = lax.broadcasted_iota(jnp.int32, (STATS, LANES), 0) + STATS
    at_lane = lax.broadcasted_iota(jnp.int32, (STATS, LANES), 1)
    line_ids = lax.broadcasted_iota(jnp.int32, (tiles, LANES), 0) * LANES
    ids = line_ids + lax.broadcasted_iota(jnp.int32, (tiles, LANES), 1)
    ids = ids + col * cols_local
    hess_ref[...] = jnp.zeros_like(hess_ref)

    def send_stats(j, b):
        rows = [jnp.sum(vec_ref[k] * b, axis=0, keepdims=True) for k in range(j)]
        rows += [jnp.zeros((1, LANES), F32)] * (NB - j)
        rows.append(jnp.sum(b * b, axis=0, keepdims=True))
        rows += [jnp.zeros((1, LANES), F32)] * (STATS - NB - 1)
        sums = jnp.sum(jnp.concatenate(rows, axis=0), axis=1, keepdims=True)
        packed = jnp.where(at_lane == at_stat, sums, F32(0.0))
        packed = jnp.sum(packed, axis=0, keepdims=True)
        top = jnp.where(jnp.logical_and(col == 0, lane < STATS), b[0:1, :], packed)
        stat_ref[j] = top
        stats_ref[j, col] = top
        to_peers(stat_ref.at[j], stats_ref.at[j, col], stat_send, stat_sem.at[j])

    def total(ref, count):
        terms = [ref[i] for i in range(count)]
        while len(terms) > 1:
            terms = [x + y for x, y in zip(terms[::2], terms[1::2])]
        return terms[0]

    factor = [[None] * NB for _ in range(NB)]
    gram = [[None] * NB for _ in range(NB)]
    tops = []
    images = []
    for i in range(blocks):
        block_load(i).wait()
    expect(mypan_ref.at[pan_span(0)], pan_sem.at[0])
    b = mypan_ref[0]
    for j in range(NB):
        if j < last:
            matvec(j, b, lambda h: spread(
                h, part_ref.at[j, h], got_ref.at[j, col], part_send, part_sem.at[j]
            ))
            send_stats(j, b)
            if j > 0:
                publish(yvec_ref.at[j - 1], wy_ref, j - 1, y_send, y_sem)
            if 0 < j < NB // 2:
                send_pan(j + 1)
        else:
            send_stats(j, b)
            tail_ref[0] = b
            tail_ref[1] = yvec_ref[j - 1]
            matvec(j, b, lambda h: None)
            sums_ref[col] = part_ref[j]
            to_peers(part_ref.at[j], sums_ref.at[col], sum_send, sum_sem)
            own_rows(tail_ref, lambda at: ends_ref.at[at], tail_send, tail_sem)

        expect(stats_ref.at[j, pl.ds(0, ncol - 1)], stat_sem.at[j])
        stat = total(stats_ref.at[j], ncol)
        inner = [stat[:, STATS + k : STATS + k + 1] for k in range(j)]
        top = jnp.where(lane < STATS, stat, F32(0.0))
        weight = []
        for m in range(j):
            value = factor[0][m] * inner[0]
            for k in range(1, m + 1):
                value = value + factor[k][m] * inner[k]
            weight.append(value)
        for m in range(j):
            top = top - tops[m] * weight[m]
        above = jnp.where(lane <= j, top, F32(0.0))
        square = stat[:, STATS + NB : STATS + NB + 1]
        square = square - jnp.sum(above * above, axis=1, keepdims=True)
        norm = jnp.sqrt(square)
        alpha = top[:, j + 1 : j + 2]
        signed = jnp.where(alpha >= 0, norm, -norm)
        scale = 1.0 / jnp.sqrt(norm * (norm + jnp.abs(alpha)))
        u = b
        for m in range(j):
            u = u - vec_ref[m] * weight[m]
        u = jnp.where(ids > j, u, F32(0.0)) + jnp.where(ids == j + 1, signed, F32(0.0))
        u = u * scale
        vec_ref[j] = u
        if j < last:
            publish(vec_ref.at[j], refl_ref, j, v_send, v_sem)
        vtop = jnp.where(lane > j, top, F32(0.0))
        vtop = (vtop + jnp.where(lane == j + 1, signed, F32(0.0))) * scale
        couple = []
        for k in range(j):
            value = inner[k]
            for m in range(j):
                value = value - gram[k][m] * weight[m]
            fix = jnp.where(lane == j + 1, signed, F32(0.0)) - above
            value = value + jnp.sum(tops[k] * fix, axis=1, keepdims=True)
            couple.append(value * scale)
        for k in range(j):
            value = factor[k][k] * couple[k]
            for m in range(k + 1, j):
                value = value + factor[k][m] * couple[m]
            factor[k][j] = -value
            gram[k][j] = couple[k]
            gram[j][k] = couple[k]
        factor[j][j] = jnp.ones((1, 1), F32)
        gram[j][j] = jnp.full((1, 1), 2.0, F32)
        tops.append(vtop)
        hrow = jnp.where(lane == j + 1, -signed, above)
        hess_ref[j, 0, 0:1, :] = jnp.where(row == 0, hrow, F32(0.0))
        if j == 0 or 1 < j <= NB // 2:
            i = max(j, 1)
            expect(mypan_ref.at[pan_span(i)], pan_sem.at[i])
        if j < last:
            drop = jnp.zeros((tiles, LANES), F32)
            for k in range(j):
                drop = drop + images[k] * weight[k]
            for i in range(j + 1):
                drop = drop + mypan_ref[i] * top[:, i : i + 1]
            drop = (drop - mypan_ref[j + 1] * signed) * scale
            back = jnp.zeros((tiles, LANES), F32)
            for k in range(j):
                back = back + yvec_ref[k] * couple[k]
            rest = mypan_ref[j + 1]
            for k in range(j):
                rest = rest - yvec_ref[k] * tops[k][:, j + 1 : j + 2]
            pull = vtop[:, j + 1 : j + 2]
            rest = rest + (drop + back) * pull
            pull = pull * scale
            if 0 < j <= NB // 2 + 1:
                own_rows(
                    mypan_ref.at[pan_span(j - 1)],
                    lambda at: edges_ref.at[at, pan_span(j - 1)],
                    edge_send, edge_sem,
                )

            expect(got_ref.at[j], part_sem.at[j])
            image = total(got_ref.at[j], ncol)
            b = rest - image * pull
            image = image * scale - drop
            images.append(image)
            yvec_ref[j] = image - back

    mix = []
    for m in range(last):
        value = weight[m]
        for k in range(m + 1, last):
            value = value + gram[m][k] * weight[k]
        mix.append(value * scale + couple[m])
    expect(edges_ref, edge_sem)
    expect(wy_ref.at[pl.ds(0, last - 1)], y_sem)
    rest = []
    for h in range(split):
        value = edges_ref[h, NB] * signed
        for i in range(NB):
            value = value - edges_ref[h, i] * top[:, i : i + 1]
        value = value * scale
        for k in range(last - 1):
            value = value - wy_ref[k, h] * mix[k]
        rest.append(value)
    expect(refl_ref.at[pl.ds(0, last)], v_sem)
    expect(ends_ref, tail_sem)
    for h in range(split):
        at = line_ids + lane + (row * rows_local + h * cols_local)
        u = ends_ref[h, 0]
        for m in range(last):
            u = u - refl_ref[m, h] * weight[m]
        u = jnp.where(at > last, u, F32(0.0)) + jnp.where(at == NB, signed, F32(0.0))
        refl_ref[last, h] = u * scale
        wy_ref[last - 1, h] = ends_ref[h, 1]
        rest[h] = rest[h] - ends_ref[h, 1] * mix[last - 1]

    at_row = lax.broadcasted_iota(jnp.int32, (NB, NB), 0)
    at_col = lax.broadcasted_iota(jnp.int32, (NB, NB), 1)
    fac = jnp.zeros((NB, NB), F32)
    for k in range(NB):
        for m in range(k, NB):
            here = jnp.logical_and(at_row == k, at_col == m)
            fac = jnp.where(here, jnp.broadcast_to(factor[k][m], (NB, NB)), fac)
    fac_ref[...] = fac

    expect(stats_ref.at[:, pl.ds(0, ncol - 1)], stat_send)
    settle(got_ref.at[pl.ds(0, last)], part_send, home)
    settle(refl_ref.at[pl.ds(0, last)], v_send, home)
    settle(wy_ref.at[pl.ds(0, last - 1)], y_send, home)

    @pl.when(home)
    def _():
        expect(got_ref.at[pl.ds(0, NB + 1), pl.ds(0, ncol - 1)], edge_send)

    @pl.when(col == 0)
    def _():
        settle(got_ref.at[pl.ds(0, NB + 1)], pan_send, row == 0)

    others = sums_ref.at[pl.ds(0, ncol - 1)]
    expect(others, sum_sem)
    image = total(sums_ref, ncol)
    for h in range(split):
        wy_ref[last, h] = image[h] * scale + rest[h]
    expect(others, sum_send)

    @pl.when(home)
    def _():
        expect(others, tail_send)


def finish(hess_in, refl_in, wy_in, fac_in, hess_out, refl_out, wy_out, fac_out):
    split, tiles = hess_in.shape[1:3]
    for src, dst in ((hess_in, hess_out), (refl_in, refl_out), (wy_in, wy_out)):
        for h in range(split):
            for t in range(tiles):
                span = pl.ds((h * tiles + t) * LANES, LANES)
                for k in range(NB):
                    dst[k : k + 1, span] = src[k, h, t : t + 1, :]
    fac_out[...] = fac_in[...]


def shards(nrow, ncol, matrix):
    rows_local, cols_local = matrix.shape
    tiles = cols_local // LANES
    split = rows_local // cols_local
    blocks = rows_local // BLOCK
    panel = jax.ShapeDtypeStruct((NB, split, tiles, LANES), F32)
    vmem = pl.BlockSpec(memory_space=pltpu.VMEM)
    dma = pltpu.SemaphoreType.DMA
    hess, refl, wy, fac = pl.pallas_call(
        functools.partial(kernel, nrow, ncol),
        out_shape=(panel, panel, panel, jax.ShapeDtypeStruct((NB, NB), F32)),
        in_specs=[pl.BlockSpec(memory_space=pl.ANY)],
        out_specs=(vmem, vmem, vmem, vmem),
        scratch_shapes=[
            pltpu.VMEM((rows_local, cols_local), F32),
            pltpu.VMEM((rows_local, LANES), F32),
            pltpu.VMEM((NB + 1, split, tiles, LANES), F32),
            pltpu.VMEM((NB + 1, tiles, LANES), F32),
            pltpu.VMEM((NB, split, tiles, LANES), F32),
            pltpu.VMEM((NB + 1, ncol, tiles, LANES), F32),
            pltpu.VMEM((NB, 1, LANES), F32),
            pltpu.VMEM((NB, ncol, 1, LANES), F32),
            pltpu.VMEM((NB, tiles, LANES), F32),
            pltpu.VMEM((NB, tiles, LANES), F32),
            pltpu.VMEM((split, NB + 1, tiles, LANES), F32),
            pltpu.VMEM((2, tiles, LANES), F32),
            pltpu.VMEM((split, 2, tiles, LANES), F32),
            pltpu.VMEM((ncol, split, tiles, LANES), F32),
            dma((blocks,)),
            dma(()),
            dma(()),
            dma((NB // 2 + 1,)),
            dma(()),
            dma((NB,)),
            dma(()),
            dma((NB,)),
            dma(()),
            dma(()),
            dma(()),
            dma(()),
            dma(()),
            dma(()),
            dma(()),
            dma(()),
            dma(()),
            dma(()),
        ],
        compiler_params=pltpu.CompilerParams(
            collective_id=0, has_side_effects=True, vmem_limit_bytes=56 * 2**20
        ),
    )(matrix)

    flat = jax.ShapeDtypeStruct((NB, rows_local), F32)
    hess, refl, wy, fac = pl.pallas_call(
        finish,
        out_shape=(flat, flat, flat, jax.ShapeDtypeStruct((NB, NB), F32)),
        in_specs=[vmem] * 4,
        out_specs=(vmem,) * 4,
    )(hess, refl, wy, fac)
    return hess.T, refl.T, wy.T, fac


def solution(mesh):
    nrow, ncol = mesh.shape["row"], mesh.shape["col"]
    return jax.shard_map(
        functools.partial(shards, nrow, ncol),
        mesh=mesh,
        in_specs=(P("row", "col"),),
        out_specs=(P("row", None), P("row", None), P("row", None), P()),
        check_vma=False,
    )
```

```python
import functools

import jax
import jax.numpy as jnp
from jax import lax
from jax.experimental import pallas as pl
from jax.experimental.pallas import tpu as pltpu
from jax.sharding import PartitionSpec as P

NB = 8
LANES = 128
SUB = 8
STATS = 16
BLOCK = 256
F32 = jnp.float32


def kernel(
    nrow, ncol, a_hbm, hess_out, refl_out, wy_out, fac_ref,
    refl_ref, wy_ref, a_ref, first_ref, pan_ref, mypan_ref, part_ref, got_ref, stat_ref, stats_ref,
    vec_ref, yvec_ref, edges_ref, tail_ref, ends_ref, sums_ref, coef_ref,
    load_sem, first_sem, pan_send, pan_sem, stat_send, stat_sem,
    part_send, part_sem, v_send, v_sem, y_send, y_sem,
    edge_send, edge_sem, tail_send, tail_sem, sum_send, sum_sem,
):
    rows_local, cols_local = a_hbm.shape
    tiles = cols_local // LANES
    split = rows_local // cols_local
    row, col = lax.axis_index("row"), lax.axis_index("col")
    blocks = rows_local // BLOCK
    owner = col // split
    slot = col - owner * split
    home = owner == row
    last = NB - 1

    def wrap(value, bound):
        return jnp.where(value >= bound, value - bound, value)

    def far_first(count):
        return sorted(range(count), key=lambda d: -min(d, count - d))

    def block_load(i):
        span = pl.ds(i * BLOCK, BLOCK)
        return pltpu.make_async_copy(a_hbm.at[span], a_ref.at[span], load_sem.at[i])

    head = pltpu.make_async_copy(a_hbm.at[:, pl.ds(0, LANES)], first_ref, first_sem)

    @pl.when(col == 0)
    def _():
        head.start()

    for i in range(blocks):
        block_load(i).start(priority=1)

    barrier = pltpu.get_barrier_semaphore()

    def greet(to_row, to_col):
        pl.semaphore_signal(
            barrier, inc=1, device_id=(to_row, to_col),
            device_id_type=pl.DeviceIdType.MESH,
        )

    for dc in far_first(ncol)[:-1]:
        greet(owner, wrap(col + dc, ncol))

    @pl.when(jnp.logical_not(home))
    def _():
        greet(owner, col)

    for dc in far_first(ncol)[:-1]:
        greet(row, wrap(col + dc, ncol))

    def send(src, dst, send_sem, recv_sem, to_row, to_col):
        pltpu.make_async_remote_copy(
            src_ref=src, dst_ref=dst, send_sem=send_sem, recv_sem=recv_sem,
            device_id=(to_row, to_col), device_id_type=pl.DeviceIdType.MESH,
        ).start()

    def place(src, dst, send_sem, recv_sem, to_row, to_col, here):
        @pl.when(here)
        def _():
            pltpu.make_async_copy(src, dst, recv_sem).start()

        @pl.when(jnp.logical_not(here))
        def _():
            send(src, dst, send_sem, recv_sem, to_row, to_col)

    def to_peers(src, dst, send_sem, recv_sem):
        for dc in far_first(ncol)[:-1]:
            send(src, dst, send_sem, recv_sem, row, wrap(col + dc, ncol))

    def expect(ref, sem):
        pltpu.make_async_copy(ref, ref, sem).wait()

    def settle(ref, sem, here):
        count = ref.shape[1]

        @pl.when(jnp.logical_not(here))
        def _():
            expect(ref, sem)

        if count > 1:
            @pl.when(here)
            def _():
                expect(ref.at[:, pl.ds(0, count - 1)], sem)

    def spread_out(h, src, dst, send_sem, recv_sem):
        for dr in far_first(nrow)[:-1]:
            send(src, dst, send_sem, recv_sem, wrap(row + dr, nrow), row * split + h)

    def spread_here(h, src, dst, send_sem, recv_sem):
        to_col = row * split + h
        place(src, dst, send_sem, recv_sem, row, to_col, to_col == col)

    @pl.when(col == 0)
    def _():
        head.wait()
        for h in range(split):
            def turn(t, carry):
                at = pl.multiple_of(h * cols_local + t * LANES, LANES)
                block = first_ref[pl.ds(at, LANES), :].T
                for k in range(NB + 1):
                    pan_ref[k, h, pl.ds(t, 1), :] = block[k : k + 1, :]
                return carry

            lax.fori_loop(0, tiles, turn, 0)

    partners = split * nrow + ncol - 1
    pl.semaphore_wait(barrier, jnp.where(home, partners - 1, partners))

    def pan_span(i):
        return pl.ds(0, 1) if i == 0 else pl.ds(2 * i - 1, 2)

    def send_pan(i):
        @pl.when(col == 0)
        def _():
            for spread in (spread_out, spread_here):
                for h in range(split):
                    spread(
                        h, pan_ref.at[pan_span(i), h], mypan_ref.at[pan_span(i)],
                        pan_send, pan_sem.at[i],
                    )

    send_pan(0)
    send_pan(1)

    def fold(acc, h, t, j):
        part_ref[j, h, t : t + 1, :] = jnp.sum(acc.T, axis=0, keepdims=True)

    def matvec(j, vector, act):
        pieces = [
            jnp.broadcast_to(vector[t : t + 1, :], (SUB, LANES)) for t in range(tiles)
        ]

        def product(t):
            accs = []
            for s in range(LANES // SUB):
                at = pl.ds(t * LANES + s * SUB, SUB)
                acc = a_ref[at, pl.ds(0, LANES)] * pieces[0]
                for p in range(1, tiles):
                    acc = acc + a_ref[at, pl.ds(p * LANES, LANES)] * pieces[p]
                accs.append(acc)
            return jnp.concatenate(accs, axis=0)

        for h in range(split):
            for t in range(tiles):
                fold(product(h * tiles + t), h, t, j)
            act(h)

    def own_rows(src, dst, send_sem, recv_sem):
        @pl.when(home)
        def _():
            to_peers(src, dst(slot), send_sem, recv_sem)
            pltpu.make_async_copy(src, dst(slot), recv_sem).start()

    def lay_out(ref, out, k):
        for h in range(split):
            for t in range(tiles):
                span = pl.ds((h * tiles + t) * LANES, LANES)
                out[k : k + 1, span] = ref[k, h, t : t + 1, :]

    def publish(src, ref, j, send_sem, recv_sem):
        for i in range(split):
            to_col = row * split + i
            here = jnp.logical_and(home, to_col == col)
            place(src, ref.at[j, slot], send_sem, recv_sem, owner, to_col, here)

    lane = lax.broadcasted_iota(jnp.int32, (1, LANES), 1)
    at_stat = lax.broadcasted_iota(jnp.int32, (STATS, LANES), 0) + STATS
    at_lane = lax.broadcasted_iota(jnp.int32, (STATS, LANES), 1)
    line_ids = lax.broadcasted_iota(jnp.int32, (tiles, LANES), 0) * LANES
    ids = line_ids + lax.broadcasted_iota(jnp.int32, (tiles, LANES), 1)
    ids = ids + col * cols_local
    hess_out[...] = jnp.zeros_like(hess_out)

    def send_stats(j, b):
        rows = [jnp.sum(vec_ref[k] * b, axis=0, keepdims=True) for k in range(j)]
        rows += [jnp.zeros((1, LANES), F32)] * (NB - j)
        rows.append(jnp.sum(b * b, axis=0, keepdims=True))
        rows += [jnp.zeros((1, LANES), F32)] * (STATS - NB - 1)
        sums = jnp.sum(jnp.concatenate(rows, axis=0), axis=1, keepdims=True)
        packed = jnp.where(at_lane == at_stat, sums, F32(0.0))
        packed = jnp.sum(packed, axis=0, keepdims=True)
        top = jnp.where(jnp.logical_and(col == 0, lane < STATS), b[0:1, :], packed)
        stat_ref[j] = top
        stats_ref[j, col] = top
        to_peers(stat_ref.at[j], stats_ref.at[j, col], stat_send, stat_sem.at[j])

    def total(ref, count):
        terms = [ref[i] for i in range(count)]
        while len(terms) > 1:
            terms = [x + y for x, y in zip(terms[::2], terms[1::2])]
        return terms[0]

    factor = [[None] * NB for _ in range(NB)]
    gram = [[None] * NB for _ in range(NB)]
    tops = []
    images = []
    for i in range(blocks):
        block_load(i).wait()
    expect(mypan_ref.at[pan_span(0)], pan_sem.at[0])
    b = mypan_ref[0]
    for j in range(NB):
        if j < last:
            def share(spread, h):
                spread(
                    h, part_ref.at[j, h], got_ref.at[j, col], part_send, part_sem.at[j]
                )

            matvec(j, b, functools.partial(share, spread_out))
            for h in range(split):
                share(spread_here, h)
            send_stats(j, b)
            if j > 0:
                publish(yvec_ref.at[j - 1], wy_ref, j - 1, y_send, y_sem)
            if 0 < j < NB // 2:
                send_pan(j + 1)
        else:
            send_stats(j, b)
            tail_ref[0] = b
            tail_ref[1] = yvec_ref[j - 1]
            matvec(j, b, lambda h: None)
            sums_ref[col] = part_ref[j]
            to_peers(part_ref.at[j], sums_ref.at[col], sum_send, sum_sem)
            own_rows(tail_ref, lambda at: ends_ref.at[at], tail_send, tail_sem)

        expect(stats_ref.at[j, pl.ds(0, ncol - 1)], stat_sem.at[j])
        stat = total(stats_ref.at[j], ncol)
        inner = [stat[:, STATS + k : STATS + k + 1] for k in range(j)]
        top = jnp.where(lane < STATS, stat, F32(0.0))
        weight = []
        for m in range(j):
            value = factor[0][m] * inner[0]
            for k in range(1, m + 1):
                value = value + factor[k][m] * inner[k]
            weight.append(value)
        for m in range(j):
            top = top - tops[m] * weight[m]
        above = jnp.where(lane <= j, top, F32(0.0))
        square = stat[:, STATS + NB : STATS + NB + 1]
        square = square - jnp.sum(above * above, axis=1, keepdims=True)
        norm = jnp.sqrt(square)
        alpha = top[:, j + 1 : j + 2]
        signed = jnp.where(alpha >= 0, norm, -norm)
        scale = 1.0 / jnp.sqrt(norm * (norm + jnp.abs(alpha)))
        u = b
        for m in range(j):
            u = u - vec_ref[m] * weight[m]
        u = jnp.where(ids > j, u, F32(0.0)) + jnp.where(ids == j + 1, signed, F32(0.0))
        u = u * scale
        vec_ref[j] = u
        if j < last:
            publish(vec_ref.at[j], refl_ref, j, v_send, v_sem)
        vtop = jnp.where(lane > j, top, F32(0.0))
        vtop = (vtop + jnp.where(lane == j + 1, signed, F32(0.0))) * scale
        couple = []
        for k in range(j):
            value = inner[k]
            for m in range(j):
                value = value - gram[k][m] * weight[m]
            fix = jnp.where(lane == j + 1, signed, F32(0.0)) - above
            value = value + jnp.sum(tops[k] * fix, axis=1, keepdims=True)
            couple.append(value * scale)
        for k in range(j):
            value = factor[k][k] * couple[k]
            for m in range(k + 1, j):
                value = value + factor[k][m] * couple[m]
            factor[k][j] = -value
            gram[k][j] = couple[k]
            gram[j][k] = couple[k]
        factor[j][j] = jnp.ones((1, 1), F32)
        gram[j][j] = jnp.full((1, 1), 2.0, F32)
        tops.append(vtop)
        hrow = jnp.where(lane == j + 1, -signed, above)
        hess_out[j : j + 1, 0:LANES] = jnp.where(row == 0, hrow, F32(0.0))
        if j == 0 or 1 < j <= NB // 2:
            i = max(j, 1)
            expect(mypan_ref.at[pan_span(i)], pan_sem.at[i])
        if j < last:
            drop = jnp.zeros((tiles, LANES), F32)
            for k in range(j):
                drop = drop + images[k] * weight[k]
            for i in range(j + 1):
                drop = drop + mypan_ref[i] * top[:, i : i + 1]
            drop = (drop - mypan_ref[j + 1] * signed) * scale
            back = jnp.zeros((tiles, LANES), F32)
            for k in range(j):
                back = back + yvec_ref[k] * couple[k]
            rest = mypan_ref[j + 1]
            for k in range(j):
                rest = rest - yvec_ref[k] * tops[k][:, j + 1 : j + 2]
            pull = vtop[:, j + 1 : j + 2]
            rest = rest + (drop + back) * pull
            coef_ref[0] = jnp.broadcast_to(pull * scale, (tiles, LANES))
            coef_ref[1] = jnp.broadcast_to(scale, (tiles, LANES))
            coef_ref[2] = rest
            if 0 < j <= NB // 2 + 1:
                own_rows(
                    mypan_ref.at[pan_span(j - 1)],
                    lambda at: edges_ref.at[at, pan_span(j - 1)],
                    edge_send, edge_sem,
                )

            expect(got_ref.at[j], part_sem.at[j])
            image = total(got_ref.at[j], ncol)
            b = coef_ref[2] - image * coef_ref[0]
            image = image * coef_ref[1] - drop
            images.append(image)
            yvec_ref[j] = image - back

    mix = []
    for m in range(last):
        value = weight[m]
        for k in range(m + 1, last):
            value = value + gram[m][k] * weight[k]
        mix.append(value * scale + couple[m])
    expect(edges_ref, edge_sem)
    expect(wy_ref.at[pl.ds(0, last - 1)], y_sem)
    rest = []
    for h in range(split):
        value = edges_ref[h, NB] * signed
        for i in range(NB):
            value = value - edges_ref[h, i] * top[:, i : i + 1]
        value = value * scale
        for k in range(last - 1):
            value = value - wy_ref[k, h] * mix[k]
        rest.append(value)
    expect(refl_ref.at[pl.ds(0, last)], v_sem)
    expect(ends_ref, tail_sem)
    for h in range(split):
        at = line_ids + lane + (row * rows_local + h * cols_local)
        u = ends_ref[h, 0]
        for m in range(last):
            u = u - refl_ref[m, h] * weight[m]
        u = jnp.where(at > last, u, F32(0.0)) + jnp.where(at == NB, signed, F32(0.0))
        refl_ref[last, h] = u * scale
        wy_ref[last - 1, h] = ends_ref[h, 1]
        rest[h] = rest[h] - ends_ref[h, 1] * mix[last - 1]

    at_row = lax.broadcasted_iota(jnp.int32, (NB, NB), 0)
    at_col = lax.broadcasted_iota(jnp.int32, (NB, NB), 1)
    fac = jnp.zeros((NB, NB), F32)
    for k in range(NB):
        for m in range(k, NB):
            here = jnp.logical_and(at_row == k, at_col == m)
            fac = jnp.where(here, jnp.broadcast_to(factor[k][m], (NB, NB)), fac)
    fac_ref[...] = fac

    expect(stats_ref.at[:, pl.ds(0, ncol - 1)], stat_send)
    settle(got_ref.at[pl.ds(0, last)], part_send, home)
    settle(refl_ref.at[pl.ds(0, last)], v_send, home)
    settle(wy_ref.at[pl.ds(0, last - 1)], y_send, home)

    @pl.when(home)
    def _():
        expect(got_ref.at[pl.ds(0, NB + 1), pl.ds(0, ncol - 1)], edge_send)

    @pl.when(col == 0)
    def _():
        settle(got_ref.at[pl.ds(0, NB + 1)], pan_send, row == 0)

    for k in range(NB):
        lay_out(refl_ref, refl_out, k)
    for k in range(last):
        lay_out(wy_ref, wy_out, k)
    others = sums_ref.at[pl.ds(0, ncol - 1)]
    expect(others, sum_sem)
    image = total(sums_ref, ncol)
    for h in range(split):
        wy_ref[last, h] = image[h] * scale + rest[h]
    lay_out(wy_ref, wy_out, last)
    expect(others, sum_send)

    @pl.when(home)
    def _():
        expect(others, tail_send)


def finish(*refs):
    count = len(refs) // 2
    sems = refs[-1]
    copies = [
        pltpu.make_async_copy(refs[i], refs[count + i], sems.at[i]) for i in range(count)
    ]
    for copy in copies:
        copy.start()
    for copy in copies:
        copy.wait()


def shards(nrow, ncol, matrix):
    rows_local, cols_local = matrix.shape
    tiles = cols_local // LANES
    split = rows_local // cols_local
    blocks = rows_local // BLOCK
    panel = pltpu.VMEM((NB, rows_local), F32)
    vmem = pl.BlockSpec(memory_space=pltpu.VMEM)
    dma = pltpu.SemaphoreType.DMA
    hess, refl, wy, fac = pl.pallas_call(
        functools.partial(kernel, nrow, ncol),
        out_shape=(panel, panel, panel, pltpu.VMEM((NB, NB), F32)),
        in_specs=[pl.BlockSpec(memory_space=pl.ANY)],
        out_specs=(vmem, vmem, vmem, vmem),
        scratch_shapes=[
            pltpu.VMEM((NB, split, tiles, LANES), F32),
            pltpu.VMEM((NB, split, tiles, LANES), F32),
            pltpu.VMEM((rows_local, cols_local), F32),
            pltpu.VMEM((rows_local, LANES), F32),
            pltpu.VMEM((NB + 1, split, tiles, LANES), F32),
            pltpu.VMEM((NB + 1, tiles, LANES), F32),
            pltpu.VMEM((NB, split, tiles, LANES), F32),
            pltpu.VMEM((NB + 1, ncol, tiles, LANES), F32),
            pltpu.VMEM((NB, 1, LANES), F32),
            pltpu.VMEM((NB, ncol, 1, LANES), F32),
            pltpu.VMEM((NB, tiles, LANES), F32),
            pltpu.VMEM((NB, tiles, LANES), F32),
            pltpu.VMEM((split, NB + 1, tiles, LANES), F32),
            pltpu.VMEM((2, tiles, LANES), F32),
            pltpu.VMEM((split, 2, tiles, LANES), F32),
            pltpu.VMEM((ncol, split, tiles, LANES), F32),
            pltpu.VMEM((3, tiles, LANES), F32),
            dma((blocks,)),
            dma(()),
            dma(()),
            dma((NB // 2 + 1,)),
            dma(()),
            dma((NB,)),
            dma(()),
            dma((NB,)),
            dma(()),
            dma(()),
            dma(()),
            dma(()),
            dma(()),
            dma(()),
            dma(()),
            dma(()),
            dma(()),
            dma(()),
        ],
        compiler_params=pltpu.CompilerParams(
            collective_id=0, has_side_effects=True, vmem_limit_bytes=56 * 2**20
        ),
    )(matrix)
    made = [
        pltpu.with_memory_space_constraint(x, pltpu.VMEM) for x in (hess, refl, wy, fac)
    ]
    hess, refl, wy, fac = pl.pallas_call(
        finish,
        out_shape=[jax.ShapeDtypeStruct(x.shape, F32) for x in made],
        in_specs=[vmem] * 4,
        out_specs=[pl.BlockSpec(memory_space=pl.ANY)] * 4,
        scratch_shapes=[dma((4,))],
    )(*made)
    return hess.T, refl.T, wy.T, fac


def solution(mesh):
    nrow, ncol = mesh.shape["row"], mesh.shape["col"]
    return jax.shard_map(
        functools.partial(shards, nrow, ncol),
        mesh=mesh,
        in_specs=(P("row", "col"),),
        out_specs=(P("row", None), P("row", None), P("row", None), P()),
        check_vma=False,
    )
```

```python
import functools

import jax
import jax.numpy as jnp
from jax import lax
from jax.experimental import pallas as pl
from jax.experimental.pallas import tpu as pltpu
from jax.sharding import PartitionSpec as P

NB = 8
LANES = 128
SUB = 8
STATS = 16
BLOCK = 256
CORES = 2
CHIPS_X = 4
F32 = jnp.float32


def kernel(
    nrow, ncol, a_hbm, hess_out, refl_out, wy_out, fac_ref,
    refl_ref, wy_ref, a_ref, first_ref, pan_ref, mypan_ref, part_ref, got_ref, stat_ref, stats_ref,
    vec_ref, yvec_ref, edges_ref, tail_ref, ends_ref, sums_ref, coef_ref, relay_ref,
    load_sem, first_sem, pan_send, pan_sem, stat_send, stat_sem,
    part_send, part_sem, v_send, v_sem, y_send, y_sem,
    edge_send, edge_sem, tail_send, tail_sem, sum_send, sum_sem,
    head_send, relay_sem, kid_send, go_sem,
):
    rows_local, cols_local = a_hbm.shape
    tiles = cols_local // LANES
    split = rows_local // cols_local
    row, col = lax.axis_index("row"), lax.axis_index("col")
    blocks = rows_local // BLOCK
    owner = col // split
    slot = col - owner * split
    home = owner == row
    last = NB - 1
    rows_y, rows_z = nrow // CORES, ncol // CHIPS_X
    y, z = row // CORES, col // CHIPS_X
    core, x = row - y * CORES, col - z * CHIPS_X
    edge = rows_y - 1
    source = col == 0
    stand_in = col == 1
    near = z < rows_z // 2
    relay = near & (col > 0) & (y < edge)
    kid_col = (rows_z - 1 - z) * CHIPS_X + x
    near_y = y < rows_z // 2
    corner = (y == edge) & (core == 0)

    def wrap(value, bound):
        return jnp.where(value >= bound, value - bound, value)

    def far_first(count):
        return sorted(range(count), key=lambda d: -min(d, count - d))

    def block_load(i):
        span = pl.ds(i * BLOCK, BLOCK)
        return pltpu.make_async_copy(a_hbm.at[span], a_ref.at[span], load_sem.at[i])

    head = pltpu.make_async_copy(a_hbm.at[:, pl.ds(0, LANES)], first_ref, first_sem)

    @pl.when(col == 0)
    def _():
        head.start()

    for i in range(blocks):
        block_load(i).start(priority=1)

    barrier = pltpu.get_barrier_semaphore()

    def greet(to_row, to_col):
        pl.semaphore_signal(
            barrier, inc=1, device_id=(to_row, to_col),
            device_id_type=pl.DeviceIdType.MESH,
        )

    @pl.when(jnp.logical_not(near))
    def _():
        via_x = jnp.where((z == rows_z - 1) & (x == 0), 1, x)
        via_y = jnp.where(y == edge, 0, y)
        greet(via_y * CORES + core, (rows_z - 1 - z) * CHIPS_X + via_x)

    @pl.when(near & jnp.logical_not(home & source))
    def _():
        greet(owner, 0)

    @pl.when(relay)
    def _():
        greet(kid_col // split, 0)

    def greet_for(to_row, dc):
        to_col = wrap(col + dc, ncol)
        greet(to_row, jnp.where(to_col == 0, 1, to_col))

    for dc in range(1, ncol - 1):
        greet_for(owner, dc)

    @pl.when(jnp.logical_not(stand_in & home))
    def _():
        greet_for(owner, ncol - 1)

    @pl.when(jnp.logical_not(home))
    def _():
        greet_for(owner, 0)

    for dc in range(1, ncol - 1):
        greet_for(row, dc)

    @pl.when(jnp.logical_not(stand_in))
    def _():
        greet_for(row, ncol - 1)

    def send(src, dst, send_sem, recv_sem, to_row, to_col):
        pltpu.make_async_remote_copy(
            src_ref=src, dst_ref=dst, send_sem=send_sem, recv_sem=recv_sem,
            device_id=(to_row, to_col), device_id_type=pl.DeviceIdType.MESH,
        ).start()

    def place(src, dst, send_sem, recv_sem, to_row, to_col, here):
        @pl.when(here)
        def _():
            pltpu.make_async_copy(src, dst, recv_sem).start()

        @pl.when(jnp.logical_not(here))
        def _():
            send(src, dst, send_sem, recv_sem, to_row, to_col)

    def to_peers(src, dst, send_sem, recv_sem):
        for dc in far_first(ncol)[:-1]:
            send(src, dst, send_sem, recv_sem, row, wrap(col + dc, ncol))

    def expect(ref, sem):
        pltpu.make_async_copy(ref, ref, sem).wait()

    def settle(ref, sem, here):
        count = ref.shape[1]

        @pl.when(jnp.logical_not(here))
        def _():
            expect(ref, sem)

        if count > 1:
            @pl.when(here)
            def _():
                expect(ref.at[:, pl.ds(0, count - 1)], sem)

    def spread_out(h, src, dst, send_sem, recv_sem):
        for dr in far_first(nrow)[:-1]:
            send(src, dst, send_sem, recv_sem, wrap(row + dr, nrow), row * split + h)

    def spread_here(h, src, dst, send_sem, recv_sem):
        to_col = row * split + h
        place(src, dst, send_sem, recv_sem, row, to_col, to_col == col)

    @pl.when(col == 0)
    def _():
        head.wait()
        for h in range(split):
            def turn(t, carry):
                at = pl.multiple_of(h * cols_local + t * LANES, LANES)
                block = first_ref[pl.ds(at, LANES), :].T
                for k in range(NB + 1):
                    pan_ref[k, h, pl.ds(t, 1), :] = block[k : k + 1, :]
                return carry

            lax.fori_loop(0, tiles, turn, 0)

    one = jnp.where(home, 1, 0)
    partners = split * nrow + ncol - 1 - one
    kids = jnp.where(stand_in, 2, 1) * jnp.where(y == 0, 2, 1)
    proxied = jnp.where(stand_in, split * nrow + ncol - 2 - 2 * one, 0)
    others = partners + proxied + jnp.where(relay, kids, 0)
    via = (nrow - CORES) * jnp.where(corner, 1, split)
    first = jnp.where(near_y, split * nrow - one, via)
    pl.semaphore_wait(barrier, jnp.where(source, first, others))

    @pl.when(stand_in)
    def _():
        pl.semaphore_signal(
            go_sem, inc=1, device_id=(row, col - 1),
            device_id_type=pl.DeviceIdType.MESH,
        )

    def pan_span(i):
        return pl.ds(0, 1) if i == 0 else pl.ds(2 * i - 1, 2)

    def send_pan(i):
        @pl.when(col == 0)
        def _():
            for spread in (spread_out, spread_here):
                for h in range(split):
                    spread(
                        h, pan_ref.at[pan_span(i), h], mypan_ref.at[pan_span(i)],
                        pan_send, pan_sem.at[i],
                    )

    head_span = pl.ds(0, 1)

    @pl.when(source & near_y)
    def _():
        for spread in (spread_out, spread_here):
            for h in range(split):
                spread(
                    h, pan_ref.at[head_span, h], mypan_ref.at[head_span],
                    head_send, pan_sem.at[0],
                )

    @pl.when(source & jnp.logical_not(near_y))
    def _():
        for to_row in range(nrow - CORES):
            for h in range(split):
                to_x = core * split + h
                moved = jnp.where((y == edge) & (to_x == 0), 1, 0)
                send(
                    pan_ref.at[head_span, h], relay_ref.at[pl.ds(moved, 1)],
                    head_send, relay_sem,
                    to_row, (rows_z - 1 - y) * CHIPS_X + to_x + moved,
                )

    def hand_on(act):
        for i in range(2):
            @pl.when(relay if i == 0 else relay & stand_in)
            def _():
                act(2 * i, row, kid_col - i)

                @pl.when(y == 0)
                def _():
                    act(2 * i + 1, edge * CORES + core, kid_col - i)

    def hand(i, to_row, to_col):
        send(
            relay_ref.at[pl.ds(i // 2, 1)], mypan_ref.at[head_span],
            kid_send.at[i], pan_sem.at[0], to_row, to_col,
        )

    @pl.when(relay & stand_in)
    def _():
        expect(relay_ref, relay_sem)

    @pl.when(relay & jnp.logical_not(stand_in))
    def _():
        expect(relay_ref.at[head_span], relay_sem)

    hand_on(hand)

    @pl.when(source)
    def _():
        pl.semaphore_wait(go_sem, 1)

    send_pan(1)

    def fold(acc, h, t, j):
        part_ref[j, h, t : t + 1, :] = jnp.sum(acc.T, axis=0, keepdims=True)

    def matvec(j, vector, act):
        pieces = [
            jnp.broadcast_to(vector[t : t + 1, :], (SUB, LANES)) for t in range(tiles)
        ]

        def product(t):
            accs = []
            for s in range(LANES // SUB):
                at = pl.ds(t * LANES + s * SUB, SUB)
                acc = a_ref[at, pl.ds(0, LANES)] * pieces[0]
                for p in range(1, tiles):
                    acc = acc + a_ref[at, pl.ds(p * LANES, LANES)] * pieces[p]
                accs.append(acc)
            return jnp.concatenate(accs, axis=0)

        for h in range(split):
            for t in range(tiles):
                fold(product(h * tiles + t), h, t, j)
            act(h)

    def own_rows(src, dst, send_sem, recv_sem):
        @pl.when(home)
        def _():
            to_peers(src, dst(slot), send_sem, recv_sem)
            pltpu.make_async_copy(src, dst(slot), recv_sem).start()

    def lay_out(ref, out, k):
        for h in range(split):
            for t in range(tiles):
                span = pl.ds((h * tiles + t) * LANES, LANES)
                out[k : k + 1, span] = ref[k, h, t : t + 1, :]

    def publish(src, ref, j, send_sem, recv_sem):
        for i in range(split):
            to_col = row * split + i
            here = jnp.logical_and(home, to_col == col)
            place(src, ref.at[j, slot], send_sem, recv_sem, owner, to_col, here)

    lane = lax.broadcasted_iota(jnp.int32, (1, LANES), 1)
    at_stat = lax.broadcasted_iota(jnp.int32, (STATS, LANES), 0) + STATS
    at_lane = lax.broadcasted_iota(jnp.int32, (STATS, LANES), 1)
    line_ids = lax.broadcasted_iota(jnp.int32, (tiles, LANES), 0) * LANES
    ids = line_ids + lax.broadcasted_iota(jnp.int32, (tiles, LANES), 1)
    ids = ids + col * cols_local
    hess_out[...] = jnp.zeros_like(hess_out)

    def send_stats(j, b):
        rows = [jnp.sum(vec_ref[k] * b, axis=0, keepdims=True) for k in range(j)]
        rows += [jnp.zeros((1, LANES), F32)] * (NB - j)
        rows.append(jnp.sum(b * b, axis=0, keepdims=True))
        rows += [jnp.zeros((1, LANES), F32)] * (STATS - NB - 1)
        sums = jnp.sum(jnp.concatenate(rows, axis=0), axis=1, keepdims=True)
        packed = jnp.where(at_lane == at_stat, sums, F32(0.0))
        packed = jnp.sum(packed, axis=0, keepdims=True)
        top = jnp.where(jnp.logical_and(col == 0, lane < STATS), b[0:1, :], packed)
        stat_ref[j] = top
        stats_ref[j, col] = top
        to_peers(stat_ref.at[j], stats_ref.at[j, col], stat_send, stat_sem.at[j])

    def total(ref, count):
        terms = [ref[i] for i in range(count)]
        while len(terms) > 1:
            terms = [x + y for x, y in zip(terms[::2], terms[1::2])]
        return terms[0]

    factor = [[None] * NB for _ in range(NB)]
    gram = [[None] * NB for _ in range(NB)]
    tops = []
    images = []
    for i in range(blocks):
        block_load(i).wait()
    expect(mypan_ref.at[pan_span(0)], pan_sem.at[0])
    b = mypan_ref[0]
    for j in range(NB):
        if j < last:
            def share(spread, h):
                spread(
                    h, part_ref.at[j, h], got_ref.at[j, col], part_send, part_sem.at[j]
                )

            matvec(j, b, functools.partial(share, spread_out))
            for h in range(split):
                share(spread_here, h)
            send_stats(j, b)
            if j > 0:
                publish(yvec_ref.at[j - 1], wy_ref, j - 1, y_send, y_sem)
            if 0 < j < NB // 2:
                send_pan(j + 1)
        else:
            send_stats(j, b)
            tail_ref[0] = b
            tail_ref[1] = yvec_ref[j - 1]
            matvec(j, b, lambda h: None)
            sums_ref[col] = part_ref[j]
            to_peers(part_ref.at[j], sums_ref.at[col], sum_send, sum_sem)
            own_rows(tail_ref, lambda at: ends_ref.at[at], tail_send, tail_sem)

        expect(stats_ref.at[j, pl.ds(0, ncol - 1)], stat_sem.at[j])
        stat = total(stats_ref.at[j], ncol)
        inner = [stat[:, STATS + k : STATS + k + 1] for k in range(j)]
        top = jnp.where(lane < STATS, stat, F32(0.0))
        weight = []
        for m in range(j):
            value = factor[0][m] * inner[0]
            for k in range(1, m + 1):
                value = value + factor[k][m] * inner[k]
            weight.append(value)
        for m in range(j):
            top = top - tops[m] * weight[m]
        above = jnp.where(lane <= j, top, F32(0.0))
        square = stat[:, STATS + NB : STATS + NB + 1]
        square = square - jnp.sum(above * above, axis=1, keepdims=True)
        norm = jnp.sqrt(square)
        alpha = top[:, j + 1 : j + 2]
        signed = jnp.where(alpha >= 0, norm, -norm)
        scale = 1.0 / jnp.sqrt(norm * (norm + jnp.abs(alpha)))
        u = b
        for m in range(j):
            u = u - vec_ref[m] * weight[m]
        u = jnp.where(ids > j, u, F32(0.0)) + jnp.where(ids == j + 1, signed, F32(0.0))
        u = u * scale
        vec_ref[j] = u
        if j < last:
            publish(vec_ref.at[j], refl_ref, j, v_send, v_sem)
        vtop = jnp.where(lane > j, top, F32(0.0))
        vtop = (vtop + jnp.where(lane == j + 1, signed, F32(0.0))) * scale
        couple = []
        for k in range(j):
            value = inner[k]
            for m in range(j):
                value = value - gram[k][m] * weight[m]
            fix = jnp.where(lane == j + 1, signed, F32(0.0)) - above
            value = value + jnp.sum(tops[k] * fix, axis=1, keepdims=True)
            couple.append(value * scale)
        for k in range(j):
            value = factor[k][k] * couple[k]
            for m in range(k + 1, j):
                value = value + factor[k][m] * couple[m]
            factor[k][j] = -value
            gram[k][j] = couple[k]
            gram[j][k] = couple[k]
        factor[j][j] = jnp.ones((1, 1), F32)
        gram[j][j] = jnp.full((1, 1), 2.0, F32)
        tops.append(vtop)
        hrow = jnp.where(lane == j + 1, -signed, above)
        hess_out[j : j + 1, 0:LANES] = jnp.where(row == 0, hrow, F32(0.0))
        if j == 0 or 1 < j <= NB // 2:
            i = max(j, 1)
            expect(mypan_ref.at[pan_span(i)], pan_sem.at[i])
        if j < last:
            drop = jnp.zeros((tiles, LANES), F32)
            for k in range(j):
                drop = drop + images[k] * weight[k]
            for i in range(j + 1):
                drop = drop + mypan_ref[i] * top[:, i : i + 1]
            drop = (drop - mypan_ref[j + 1] * signed) * scale
            back = jnp.zeros((tiles, LANES), F32)
            for k in range(j):
                back = back + yvec_ref[k] * couple[k]
            rest = mypan_ref[j + 1]
            for k in range(j):
                rest = rest - yvec_ref[k] * tops[k][:, j + 1 : j + 2]
            pull = vtop[:, j + 1 : j + 2]
            rest = rest + (drop + back) * pull
            coef_ref[0] = jnp.broadcast_to(pull * scale, (tiles, LANES))
            coef_ref[1] = jnp.broadcast_to(scale, (tiles, LANES))
            coef_ref[2] = rest
            if 0 < j <= NB // 2 + 1:
                own_rows(
                    mypan_ref.at[pan_span(j - 1)],
                    lambda at: edges_ref.at[at, pan_span(j - 1)],
                    edge_send, edge_sem,
                )

            expect(got_ref.at[j], part_sem.at[j])
            image = total(got_ref.at[j], ncol)
            b = coef_ref[2] - image * coef_ref[0]
            image = image * coef_ref[1] - drop
            images.append(image)
            yvec_ref[j] = image - back

    mix = []
    for m in range(last):
        value = weight[m]
        for k in range(m + 1, last):
            value = value + gram[m][k] * weight[k]
        mix.append(value * scale + couple[m])
    expect(edges_ref, edge_sem)
    expect(wy_ref.at[pl.ds(0, last - 1)], y_sem)
    rest = []
    for h in range(split):
        value = edges_ref[h, NB] * signed
        for i in range(NB):
            value = value - edges_ref[h, i] * top[:, i : i + 1]
        value = value * scale
        for k in range(last - 1):
            value = value - wy_ref[k, h] * mix[k]
        rest.append(value)
    expect(refl_ref.at[pl.ds(0, last)], v_sem)
    expect(ends_ref, tail_sem)
    for h in range(split):
        at = line_ids + lane + (row * rows_local + h * cols_local)
        u = ends_ref[h, 0]
        for m in range(last):
            u = u - refl_ref[m, h] * weight[m]
        u = jnp.where(at > last, u, F32(0.0)) + jnp.where(at == NB, signed, F32(0.0))
        refl_ref[last, h] = u * scale
        wy_ref[last - 1, h] = ends_ref[h, 1]
        rest[h] = rest[h] - ends_ref[h, 1] * mix[last - 1]

    at_row = lax.broadcasted_iota(jnp.int32, (NB, NB), 0)
    at_col = lax.broadcasted_iota(jnp.int32, (NB, NB), 1)
    fac = jnp.zeros((NB, NB), F32)
    for k in range(NB):
        for m in range(k, NB):
            here = jnp.logical_and(at_row == k, at_col == m)
            fac = jnp.where(here, jnp.broadcast_to(factor[k][m], (NB, NB)), fac)
    fac_ref[...] = fac

    expect(stats_ref.at[:, pl.ds(0, ncol - 1)], stat_send)
    settle(got_ref.at[pl.ds(0, last)], part_send, home)
    settle(refl_ref.at[pl.ds(0, last)], v_send, home)
    settle(wy_ref.at[pl.ds(0, last - 1)], y_send, home)

    @pl.when(home)
    def _():
        expect(got_ref.at[pl.ds(0, NB + 1), pl.ds(0, ncol - 1)], edge_send)

    hand_on(lambda i, to_row, to_col: expect(relay_ref.at[head_span], kid_send.at[i]))

    @pl.when(source)
    def _():
        settle(got_ref.at[pl.ds(0, NB)], pan_send, row == 0)

    @pl.when(source & near_y)
    def _():
        settle(got_ref.at[pl.ds(0, 1)], head_send, row == 0)

    @pl.when(source & jnp.logical_not(near_y))
    def _():
        expect(got_ref.at[0, pl.ds(0, split * (nrow - CORES))], head_send)

    for k in range(NB):
        lay_out(refl_ref, refl_out, k)
    for k in range(last):
        lay_out(wy_ref, wy_out, k)
    others = sums_ref.at[pl.ds(0, ncol - 1)]
    expect(others, sum_sem)
    image = total(sums_ref, ncol)
    for h in range(split):
        wy_ref[last, h] = image[h] * scale + rest[h]
    lay_out(wy_ref, wy_out, last)
    expect(others, sum_send)

    @pl.when(home)
    def _():
        expect(others, tail_send)


def finish(*refs):
    count = len(refs) // 2
    sems = refs[-1]
    copies = [
        pltpu.make_async_copy(refs[i], refs[count + i], sems.at[i]) for i in range(count)
    ]
    for copy in copies:
        copy.start()
    for copy in copies:
        copy.wait()


def shards(nrow, ncol, matrix):
    rows_local, cols_local = matrix.shape
    tiles = cols_local // LANES
    split = rows_local // cols_local
    blocks = rows_local // BLOCK
    panel = pltpu.VMEM((NB, rows_local), F32)
    vmem = pl.BlockSpec(memory_space=pltpu.VMEM)
    dma = pltpu.SemaphoreType.DMA
    hess, refl, wy, fac = pl.pallas_call(
        functools.partial(kernel, nrow, ncol),
        out_shape=(panel, panel, panel, pltpu.VMEM((NB, NB), F32)),
        in_specs=[pl.BlockSpec(memory_space=pl.ANY)],
        out_specs=(vmem, vmem, vmem, vmem),
        scratch_shapes=[
            pltpu.VMEM((NB, split, tiles, LANES), F32),
            pltpu.VMEM((NB, split, tiles, LANES), F32),
            pltpu.VMEM((rows_local, cols_local), F32),
            pltpu.VMEM((rows_local, LANES), F32),
            pltpu.VMEM((NB + 1, split, tiles, LANES), F32),
            pltpu.VMEM((NB + 1, tiles, LANES), F32),
            pltpu.VMEM((NB, split, tiles, LANES), F32),
            pltpu.VMEM((NB + 1, ncol, tiles, LANES), F32),
            pltpu.VMEM((NB, 1, LANES), F32),
            pltpu.VMEM((NB, ncol, 1, LANES), F32),
            pltpu.VMEM((NB, tiles, LANES), F32),
            pltpu.VMEM((NB, tiles, LANES), F32),
            pltpu.VMEM((split, NB + 1, tiles, LANES), F32),
            pltpu.VMEM((2, tiles, LANES), F32),
            pltpu.VMEM((split, 2, tiles, LANES), F32),
            pltpu.VMEM((ncol, split, tiles, LANES), F32),
            pltpu.VMEM((3, tiles, LANES), F32),
            pltpu.VMEM((2, tiles, LANES), F32),
            dma((blocks,)),
            dma(()),
            dma(()),
            dma((NB // 2 + 1,)),
            dma(()),
            dma((NB,)),
            dma(()),
            dma((NB,)),
            dma(()),
            dma(()),
            dma(()),
            dma(()),
            dma(()),
            dma(()),
            dma(()),
            dma(()),
            dma(()),
            dma(()),
            dma(()),
            dma(()),
            dma((4,)),
            pltpu.SemaphoreType.REGULAR,
        ],
        compiler_params=pltpu.CompilerParams(
            collective_id=0, has_side_effects=True, vmem_limit_bytes=56 * 2**20
        ),
    )(matrix)
    made = [
        pltpu.with_memory_space_constraint(x, pltpu.VMEM) for x in (hess, refl, wy, fac)
    ]
    hess, refl, wy, fac = pl.pallas_call(
        finish,
        out_shape=[jax.ShapeDtypeStruct(x.shape, F32) for x in made],
        in_specs=[vmem] * 4,
        out_specs=[pl.BlockSpec(memory_space=pl.ANY)] * 4,
        scratch_shapes=[dma((4,))],
    )(*made)
    return hess.T, refl.T, wy.T, fac


def solution(mesh):
    nrow, ncol = mesh.shape["row"], mesh.shape["col"]
    return jax.shard_map(
        functools.partial(shards, nrow, ncol),
        mesh=mesh,
        in_specs=(P("row", "col"),),
        out_specs=(P("row", None), P("row", None), P("row", None), P()),
        check_vma=False,
    )
```

```python
import functools

import jax
import jax.numpy as jnp
from jax import lax
from jax.experimental import pallas as pl
from jax.experimental.pallas import tpu as pltpu
from jax.sharding import PartitionSpec as P

NB = 8
LANES = 128
SUB = 8
STATS = 16
BLOCK = 256
CORES = 2
CHIPS_X = 4
F32 = jnp.float32


def kernel(
    nrow, ncol, a_hbm, hess_out, refl_out, wy_out, fac_ref,
    refl_ref, wy_ref, a_ref, first_ref, pan_ref, mypan_ref, part_ref, got_ref, stat_ref, stats_ref,
    vec_ref, yvec_ref, edges_ref, tail_ref, ends_ref, sums_ref, coef_ref, relay_ref,
    load_sem, first_sem, pan_send, pan_sem, stat_send, stat_sem,
    part_send, part_sem, v_send, v_sem, y_send, y_sem,
    edge_send, edge_sem, tail_send, tail_sem, sum_send, sum_sem,
    head_send, relay_sem, kid_send, go_sem,
):
    rows_local, cols_local = a_hbm.shape
    tiles = cols_local // LANES
    split = rows_local // cols_local
    row, col = lax.axis_index("row"), lax.axis_index("col")
    blocks = rows_local // BLOCK
    owner = col // split
    slot = col - owner * split
    home = owner == row
    last = NB - 1
    planes = ncol // CHIPS_X
    y, z = row // CORES, col // CHIPS_X
    core, x = row - y * CORES, col - z * CHIPS_X
    front = z == 0
    source = col == 0
    relay = front & (col > 0)
    stand_in = z == 1
    twice = col == 1

    def wrap(value, bound):
        return jnp.where(value >= bound, value - bound, value)

    def far_first(count):
        return sorted(range(count), key=lambda d: -min(d, count - d))

    def block_load(i):
        span = pl.ds(i * BLOCK, BLOCK)
        return pltpu.make_async_copy(a_hbm.at[span], a_ref.at[span], load_sem.at[i])

    head = pltpu.make_async_copy(a_hbm.at[:, pl.ds(0, LANES)], first_ref, first_sem)

    @pl.when(col == 0)
    def _():
        head.start()

    for i in range(blocks):
        block_load(i).start(priority=1)

    barrier = pltpu.get_barrier_semaphore()

    def greet(to_row, to_col):
        pl.semaphore_signal(
            barrier, inc=1, device_id=(to_row, to_col),
            device_id_type=pl.DeviceIdType.MESH,
        )

    @pl.when(jnp.logical_not(front))
    def _():
        greet(row, jnp.where(x == 0, 1, x))

    @pl.when(front & jnp.logical_not(home & source))
    def _():
        greet(owner, 0)

    @pl.when(relay)
    def _():
        for plane in range(1, planes):
            greet(plane * CORES + owner, 0)

    def greet_for(to_row, dc):
        to_col = wrap(col + dc, ncol)
        greet(to_row, jnp.where(to_col < CHIPS_X, to_col + CHIPS_X, to_col))

    behind = ncol - CHIPS_X
    for to_row, skip in ((owner, stand_in & home), (row, stand_in)):
        for dc in range(1, ncol):
            if dc != behind:
                greet_for(to_row, dc)

        @pl.when(jnp.logical_not(skip))
        def _():
            greet_for(to_row, behind)

    @pl.when(jnp.logical_not(home))
    def _():
        greet_for(owner, 0)

    def send(src, dst, send_sem, recv_sem, to_row, to_col):
        pltpu.make_async_remote_copy(
            src_ref=src, dst_ref=dst, send_sem=send_sem, recv_sem=recv_sem,
            device_id=(to_row, to_col), device_id_type=pl.DeviceIdType.MESH,
        ).start()

    def place(src, dst, send_sem, recv_sem, to_row, to_col, here):
        @pl.when(here)
        def _():
            pltpu.make_async_copy(src, dst, recv_sem).start()

        @pl.when(jnp.logical_not(here))
        def _():
            send(src, dst, send_sem, recv_sem, to_row, to_col)

    def to_peers(src, dst, send_sem, recv_sem):
        for dc in far_first(ncol)[:-1]:
            send(src, dst, send_sem, recv_sem, row, wrap(col + dc, ncol))

    def expect(ref, sem):
        pltpu.make_async_copy(ref, ref, sem).wait()

    def settle(ref, sem, here):
        count = ref.shape[1]

        @pl.when(jnp.logical_not(here))
        def _():
            expect(ref, sem)

        if count > 1:
            @pl.when(here)
            def _():
                expect(ref.at[:, pl.ds(0, count - 1)], sem)

    def spread_out(h, src, dst, send_sem, recv_sem):
        for dr in far_first(nrow)[:-1]:
            send(src, dst, send_sem, recv_sem, wrap(row + dr, nrow), row * split + h)

    def spread_here(h, src, dst, send_sem, recv_sem):
        to_col = row * split + h
        place(src, dst, send_sem, recv_sem, row, to_col, to_col == col)

    @pl.when(col == 0)
    def _():
        head.wait()
        for h in range(split):
            def turn(t, carry):
                at = pl.multiple_of(h * cols_local + t * LANES, LANES)
                block = first_ref[pl.ds(at, LANES), :].T
                for k in range(NB + 1):
                    pan_ref[k, h, pl.ds(t, 1), :] = block[k : k + 1, :]
                return carry

            lax.fori_loop(0, tiles, turn, 0)

    one = jnp.where(home, 1, 0)
    partners = split * nrow + ncol - 1 - one
    front_home = jnp.where((col - CHIPS_X) // split == row, 1, 0)
    proxied = partners - 1 + one - front_home - one
    kids = (planes - 1) * jnp.where(twice, 2, 1)
    first = jnp.where(core == 0, nrow, split * nrow)
    first = jnp.where(y == 0, split * nrow - one, first)
    count = jnp.where(stand_in, partners + proxied, partners)
    count = jnp.where(source, first, jnp.where(relay, kids, count))
    pl.semaphore_wait(barrier, count)

    @pl.when(stand_in)
    def _():
        pl.semaphore_signal(
            go_sem, inc=1, device_id=(row, col - CHIPS_X),
            device_id_type=pl.DeviceIdType.MESH,
        )

    def pan_span(i):
        return pl.ds(0, 1) if i == 0 else pl.ds(2 * i - 1, 2)

    def send_pan(i):
        @pl.when(col == 0)
        def _():
            for spread in (spread_out, spread_here):
                for h in range(split):
                    spread(
                        h, pan_ref.at[pan_span(i), h], mypan_ref.at[pan_span(i)],
                        pan_send, pan_sem.at[i],
                    )

    head_span = pl.ds(0, 1)

    @pl.when(source & (y == 0))
    def _():
        for spread in (spread_out, spread_here):
            for h in range(split):
                spread(
                    h, pan_ref.at[head_span, h], mypan_ref.at[head_span],
                    head_send, pan_sem.at[0],
                )

    @pl.when(source & (y > 0))
    def _():
        for dr in far_first(nrow):
            for h in range(split):
                to_x = core * split + h
                moved = jnp.where(to_x == 0, 1, 0)
                send(
                    pan_ref.at[head_span, h], relay_ref.at[moved, pl.ds(y, 1)],
                    head_send, relay_sem.at[moved, y], wrap(row + dr, nrow), to_x + moved,
                )

    def hand_on(i):
        for plane in far_first(planes)[:-1]:
            piece = relay_ref.at[i, pl.ds(plane, 1)]
            expect(piece, relay_sem.at[i, plane])
            send(
                piece, mypan_ref.at[head_span], kid_send.at[i], pan_sem.at[0],
                row, plane * CHIPS_X + x - i,
            )

    @pl.when(relay)
    def _():
        hand_on(0)

    @pl.when(twice)
    def _():
        hand_on(1)

    @pl.when(front)
    def _():
        pl.semaphore_wait(go_sem, 1)

    send_pan(1)

    def fold(acc, h, t, j):
        part_ref[j, h, t : t + 1, :] = jnp.sum(acc.T, axis=0, keepdims=True)

    def matvec(j, vector, act):
        pieces = [
            jnp.broadcast_to(vector[t : t + 1, :], (SUB, LANES)) for t in range(tiles)
        ]

        def product(t):
            accs = []
            for s in range(LANES // SUB):
                at = pl.ds(t * LANES + s * SUB, SUB)
                acc = a_ref[at, pl.ds(0, LANES)] * pieces[0]
                for p in range(1, tiles):
                    acc = acc + a_ref[at, pl.ds(p * LANES, LANES)] * pieces[p]
                accs.append(acc)
            return jnp.concatenate(accs, axis=0)

        for h in range(split):
            for t in range(tiles):
                fold(product(h * tiles + t), h, t, j)
            act(h)

    def own_rows(src, dst, send_sem, recv_sem):
        @pl.when(home)
        def _():
            to_peers(src, dst(slot), send_sem, recv_sem)
            pltpu.make_async_copy(src, dst(slot), recv_sem).start()

    def lay_out(ref, out, k):
        for h in range(split):
            for t in range(tiles):
                span = pl.ds((h * tiles + t) * LANES, LANES)
                out[k : k + 1, span] = ref[k, h, t : t + 1, :]

    def publish(src, ref, j, send_sem, recv_sem):
        for i in range(split):
            to_col = row * split + i
            here = jnp.logical_and(home, to_col == col)
            place(src, ref.at[j, slot], send_sem, recv_sem, owner, to_col, here)

    lane = lax.broadcasted_iota(jnp.int32, (1, LANES), 1)
    at_stat = lax.broadcasted_iota(jnp.int32, (STATS, LANES), 0) + STATS
    at_lane = lax.broadcasted_iota(jnp.int32, (STATS, LANES), 1)
    line_ids = lax.broadcasted_iota(jnp.int32, (tiles, LANES), 0) * LANES
    ids = line_ids + lax.broadcasted_iota(jnp.int32, (tiles, LANES), 1)
    ids = ids + col * cols_local
    hess_out[...] = jnp.zeros_like(hess_out)

    def send_stats(j, b):
        rows = [jnp.sum(vec_ref[k] * b, axis=0, keepdims=True) for k in range(j)]
        rows += [jnp.zeros((1, LANES), F32)] * (NB - j)
        rows.append(jnp.sum(b * b, axis=0, keepdims=True))
        rows += [jnp.zeros((1, LANES), F32)] * (STATS - NB - 1)
        sums = jnp.sum(jnp.concatenate(rows, axis=0), axis=1, keepdims=True)
        packed = jnp.where(at_lane == at_stat, sums, F32(0.0))
        packed = jnp.sum(packed, axis=0, keepdims=True)
        top = jnp.where(jnp.logical_and(col == 0, lane < STATS), b[0:1, :], packed)
        stat_ref[j] = top
        stats_ref[j, col] = top
        to_peers(stat_ref.at[j], stats_ref.at[j, col], stat_send, stat_sem.at[j])

    def total(ref, count):
        terms = [ref[i] for i in range(count)]
        while len(terms) > 1:
            terms = [x + y for x, y in zip(terms[::2], terms[1::2])]
        return terms[0]

    factor = [[None] * NB for _ in range(NB)]
    gram = [[None] * NB for _ in range(NB)]
    tops = []
    images = []
    for i in range(blocks):
        block_load(i).wait()
    expect(mypan_ref.at[pan_span(0)], pan_sem.at[0])
    b = mypan_ref[0]
    for j in range(NB):
        if j < last:
            def share(spread, h):
                spread(
                    h, part_ref.at[j, h], got_ref.at[j, col], part_send, part_sem.at[j]
                )

            matvec(j, b, functools.partial(share, spread_out))
            for h in range(split):
                share(spread_here, h)
            send_stats(j, b)
            if j > 0:
                publish(yvec_ref.at[j - 1], wy_ref, j - 1, y_send, y_sem)
            if 0 < j < NB // 2:
                send_pan(j + 1)
        else:
            send_stats(j, b)
            tail_ref[0] = b
            tail_ref[1] = yvec_ref[j - 1]
            matvec(j, b, lambda h: None)
            sums_ref[col] = part_ref[j]
            to_peers(part_ref.at[j], sums_ref.at[col], sum_send, sum_sem)
            own_rows(tail_ref, lambda at: ends_ref.at[at], tail_send, tail_sem)

        expect(stats_ref.at[j, pl.ds(0, ncol - 1)], stat_sem.at[j])
        stat = total(stats_ref.at[j], ncol)
        inner = [stat[:, STATS + k : STATS + k + 1] for k in range(j)]
        top = jnp.where(lane < STATS, stat, F32(0.0))
        weight = []
        for m in range(j):
            value = factor[0][m] * inner[0]
            for k in range(1, m + 1):
                value = value + factor[k][m] * inner[k]
            weight.append(value)
        for m in range(j):
            top = top - tops[m] * weight[m]
        above = jnp.where(lane <= j, top, F32(0.0))
        square = stat[:, STATS + NB : STATS + NB + 1]
        square = square - jnp.sum(above * above, axis=1, keepdims=True)
        norm = jnp.sqrt(square)
        alpha = top[:, j + 1 : j + 2]
        signed = jnp.where(alpha >= 0, norm, -norm)
        scale = 1.0 / jnp.sqrt(norm * (norm + jnp.abs(alpha)))
        u = b
        for m in range(j):
            u = u - vec_ref[m] * weight[m]
        u = jnp.where(ids > j, u, F32(0.0)) + jnp.where(ids == j + 1, signed, F32(0.0))
        u = u * scale
        vec_ref[j] = u
        if j < last:
            publish(vec_ref.at[j], refl_ref, j, v_send, v_sem)
        vtop = jnp.where(lane > j, top, F32(0.0))
        vtop = (vtop + jnp.where(lane == j + 1, signed, F32(0.0))) * scale
        couple = []
        for k in range(j):
            value = inner[k]
            for m in range(j):
                value = value - gram[k][m] * weight[m]
            fix = jnp.where(lane == j + 1, signed, F32(0.0)) - above
            value = value + jnp.sum(tops[k] * fix, axis=1, keepdims=True)
            couple.append(value * scale)
        for k in range(j):
            value = factor[k][k] * couple[k]
            for m in range(k + 1, j):
                value = value + factor[k][m] * couple[m]
            factor[k][j] = -value
            gram[k][j] = couple[k]
            gram[j][k] = couple[k]
        factor[j][j] = jnp.ones((1, 1), F32)
        gram[j][j] = jnp.full((1, 1), 2.0, F32)
        tops.append(vtop)
        hrow = jnp.where(lane == j + 1, -signed, above)
        hess_out[j : j + 1, 0:LANES] = jnp.where(row == 0, hrow, F32(0.0))
        if j == 0 or 1 < j <= NB // 2:
            i = max(j, 1)
            expect(mypan_ref.at[pan_span(i)], pan_sem.at[i])
        if j < last:
            drop = jnp.zeros((tiles, LANES), F32)
            for k in range(j):
                drop = drop + images[k] * weight[k]
            for i in range(j + 1):
                drop = drop + mypan_ref[i] * top[:, i : i + 1]
            drop = (drop - mypan_ref[j + 1] * signed) * scale
            back = jnp.zeros((tiles, LANES), F32)
            for k in range(j):
                back = back + yvec_ref[k] * couple[k]
            rest = mypan_ref[j + 1]
            for k in range(j):
                rest = rest - yvec_ref[k] * tops[k][:, j + 1 : j + 2]
            pull = vtop[:, j + 1 : j + 2]
            rest = rest + (drop + back) * pull
            coef_ref[0] = jnp.broadcast_to(pull * scale, (tiles, LANES))
            coef_ref[1] = jnp.broadcast_to(scale, (tiles, LANES))
            coef_ref[2] = rest
            if 0 < j <= NB // 2 + 1:
                own_rows(
                    mypan_ref.at[pan_span(j - 1)],
                    lambda at: edges_ref.at[at, pan_span(j - 1)],
                    edge_send, edge_sem,
                )

            expect(got_ref.at[j], part_sem.at[j])
            image = total(got_ref.at[j], ncol)
            b = coef_ref[2] - image * coef_ref[0]
            image = image * coef_ref[1] - drop
            images.append(image)
            yvec_ref[j] = image - back

    mix = []
    for m in range(last):
        value = weight[m]
        for k in range(m + 1, last):
            value = value + gram[m][k] * weight[k]
        mix.append(value * scale + couple[m])
    expect(edges_ref, edge_sem)
    expect(wy_ref.at[pl.ds(0, last - 1)], y_sem)
    rest = []
    for h in range(split):
        value = edges_ref[h, NB] * signed
        for i in range(NB):
            value = value - edges_ref[h, i] * top[:, i : i + 1]
        value = value * scale
        for k in range(last - 1):
            value = value - wy_ref[k, h] * mix[k]
        rest.append(value)
    expect(refl_ref.at[pl.ds(0, last)], v_sem)
    expect(ends_ref, tail_sem)
    for h in range(split):
        at = line_ids + lane + (row * rows_local + h * cols_local)
        u = ends_ref[h, 0]
        for m in range(last):
            u = u - refl_ref[m, h] * weight[m]
        u = jnp.where(at > last, u, F32(0.0)) + jnp.where(at == NB, signed, F32(0.0))
        refl_ref[last, h] = u * scale
        wy_ref[last - 1, h] = ends_ref[h, 1]
        rest[h] = rest[h] - ends_ref[h, 1] * mix[last - 1]

    at_row = lax.broadcasted_iota(jnp.int32, (NB, NB), 0)
    at_col = lax.broadcasted_iota(jnp.int32, (NB, NB), 1)
    fac = jnp.zeros((NB, NB), F32)
    for k in range(NB):
        for m in range(k, NB):
            here = jnp.logical_and(at_row == k, at_col == m)
            fac = jnp.where(here, jnp.broadcast_to(factor[k][m], (NB, NB)), fac)
    fac_ref[...] = fac

    expect(stats_ref.at[:, pl.ds(0, ncol - 1)], stat_send)
    settle(got_ref.at[pl.ds(0, last)], part_send, home)
    settle(refl_ref.at[pl.ds(0, last)], v_send, home)
    settle(wy_ref.at[pl.ds(0, last - 1)], y_send, home)

    @pl.when(home)
    def _():
        expect(got_ref.at[pl.ds(0, NB + 1), pl.ds(0, ncol - 1)], edge_send)

    for i, sent in enumerate((relay, twice)):
        @pl.when(sent)
        def _():
            expect(relay_ref.at[i, pl.ds(1, planes - 1)], kid_send.at[i])

    @pl.when(source)
    def _():
        settle(got_ref.at[pl.ds(0, NB)], pan_send, row == 0)
        settle(got_ref.at[pl.ds(0, 1)], head_send, row == 0)

    for k in range(NB):
        lay_out(refl_ref, refl_out, k)
    for k in range(last):
        lay_out(wy_ref, wy_out, k)
    others = sums_ref.at[pl.ds(0, ncol - 1)]
    expect(others, sum_sem)
    image = total(sums_ref, ncol)
    for h in range(split):
        wy_ref[last, h] = image[h] * scale + rest[h]
    lay_out(wy_ref, wy_out, last)
    expect(others, sum_send)

    @pl.when(home)
    def _():
        expect(others, tail_send)


def finish(*refs):
    count = len(refs) // 2
    sems = refs[-1]
    copies = [
        pltpu.make_async_copy(refs[i], refs[count + i], sems.at[i]) for i in range(count)
    ]
    for copy in copies:
        copy.start()
    for copy in copies:
        copy.wait()


def shards(nrow, ncol, matrix):
    rows_local, cols_local = matrix.shape
    tiles = cols_local // LANES
    split = rows_local // cols_local
    blocks = rows_local // BLOCK
    panel = pltpu.VMEM((NB, rows_local), F32)
    vmem = pl.BlockSpec(memory_space=pltpu.VMEM)
    dma = pltpu.SemaphoreType.DMA
    hess, refl, wy, fac = pl.pallas_call(
        functools.partial(kernel, nrow, ncol),
        out_shape=(panel, panel, panel, pltpu.VMEM((NB, NB), F32)),
        in_specs=[pl.BlockSpec(memory_space=pl.ANY)],
        out_specs=(vmem, vmem, vmem, vmem),
        scratch_shapes=[
            pltpu.VMEM((NB, split, tiles, LANES), F32),
            pltpu.VMEM((NB, split, tiles, LANES), F32),
            pltpu.VMEM((rows_local, cols_local), F32),
            pltpu.VMEM((rows_local, LANES), F32),
            pltpu.VMEM((NB + 1, split, tiles, LANES), F32),
            pltpu.VMEM((NB + 1, tiles, LANES), F32),
            pltpu.VMEM((NB, split, tiles, LANES), F32),
            pltpu.VMEM((NB + 1, ncol, tiles, LANES), F32),
            pltpu.VMEM((NB, 1, LANES), F32),
            pltpu.VMEM((NB, ncol, 1, LANES), F32),
            pltpu.VMEM((NB, tiles, LANES), F32),
            pltpu.VMEM((NB, tiles, LANES), F32),
            pltpu.VMEM((split, NB + 1, tiles, LANES), F32),
            pltpu.VMEM((2, tiles, LANES), F32),
            pltpu.VMEM((split, 2, tiles, LANES), F32),
            pltpu.VMEM((ncol, split, tiles, LANES), F32),
            pltpu.VMEM((3, tiles, LANES), F32),
            pltpu.VMEM((2, ncol // CHIPS_X, tiles, LANES), F32),
            dma((blocks,)),
            dma(()),
            dma(()),
            dma((NB // 2 + 1,)),
            dma(()),
            dma((NB,)),
            dma(()),
            dma((NB,)),
            dma(()),
            dma(()),
            dma(()),
            dma(()),
            dma(()),
            dma(()),
            dma(()),
            dma(()),
            dma(()),
            dma(()),
            dma(()),
            dma((2, ncol // CHIPS_X)),
            dma((2,)),
            pltpu.SemaphoreType.REGULAR,
        ],
        compiler_params=pltpu.CompilerParams(
            collective_id=0, has_side_effects=True, vmem_limit_bytes=56 * 2**20
        ),
    )(matrix)
    made = [
        pltpu.with_memory_space_constraint(x, pltpu.VMEM) for x in (hess, refl, wy, fac)
    ]
    hess, refl, wy, fac = pl.pallas_call(
        finish,
        out_shape=[jax.ShapeDtypeStruct(x.shape, F32) for x in made],
        in_specs=[vmem] * 4,
        out_specs=[pl.BlockSpec(memory_space=pl.ANY)] * 4,
        scratch_shapes=[dma((4,))],
    )(*made)
    return hess.T, refl.T, wy.T, fac


def solution(mesh):
    nrow, ncol = mesh.shape["row"], mesh.shape["col"]
    return jax.shard_map(
        functools.partial(shards, nrow, ncol),
        mesh=mesh,
        in_specs=(P("row", "col"),),
        out_specs=(P("row", None), P("row", None), P("row", None), P()),
        check_vma=False,
    )
```

```python
import functools

import jax
import jax.numpy as jnp
from jax import lax
from jax.experimental import pallas as pl
from jax.experimental.pallas import tpu as pltpu
from jax.sharding import PartitionSpec as P

NB = 8
LANES = 128
SUB = 8
STATS = 16
BLOCK = 256
CORES = 2
CHIPS_X = 4
F32 = jnp.float32


def kernel(
    nrow, ncol, a_hbm, hess_out, refl_out, wy_out, fac_ref,
    refl_ref, wy_ref, a_ref, first_ref, pan_ref, mypan_ref, part_ref, got_ref, stat_ref, stats_ref,
    vec_ref, yvec_ref, edges_ref, tail_ref, ends_ref, sums_ref, coef_ref, relay_ref,
    load_sem, first_sem, pan_send, pan_sem, stat_send, stat_sem,
    part_send, part_sem, v_send, v_sem, y_send, y_sem,
    edge_send, edge_sem, tail_send, tail_sem, sum_send, sum_sem,
    head_send, relay_sem, kid_send, go_sem,
):
    rows_local, cols_local = a_hbm.shape
    tiles = cols_local // LANES
    split = rows_local // cols_local
    row, col = lax.axis_index("row"), lax.axis_index("col")
    blocks = rows_local // BLOCK
    owner = col // split
    slot = col - owner * split
    home = owner == row
    last = NB - 1
    planes = ncol // CHIPS_X
    y, z = row // CORES, col // CHIPS_X
    core, x = row - y * CORES, col - z * CHIPS_X
    front = z == 0
    source = col == 0
    relay = front & (col > 0)
    stand_in = z == 1
    twice = col == 1

    def wrap(value, bound):
        return jnp.where(value >= bound, value - bound, value)

    def far_first(count):
        return sorted(range(count), key=lambda d: -min(d, count - d))

    def block_load(i):
        span = pl.ds(i * BLOCK, BLOCK)
        return pltpu.make_async_copy(a_hbm.at[span], a_ref.at[span], load_sem.at[i])

    head = pltpu.make_async_copy(a_hbm.at[:, pl.ds(0, LANES)], first_ref, first_sem)

    @pl.when(col == 0)
    def _():
        head.start()

    for i in range(blocks):
        block_load(i).start(priority=1)

    barrier = pltpu.get_barrier_semaphore()

    def greet(to_row, to_col):
        pl.semaphore_signal(
            barrier, inc=1, device_id=(to_row, to_col),
            device_id_type=pl.DeviceIdType.MESH,
        )

    @pl.when(jnp.logical_not(front))
    def _():
        greet(row, jnp.where(x == 0, 1, x))

    @pl.when(front & jnp.logical_not(home & source))
    def _():
        greet(owner, 0)

    @pl.when(relay)
    def _():
        for plane in range(1, planes):
            greet(plane * CORES + owner, 0)

    def greet_for(to_row, dc):
        to_col = wrap(col + dc, ncol)
        greet(to_row, jnp.where(to_col < CHIPS_X, to_col + CHIPS_X, to_col))

    behind = ncol - CHIPS_X
    for to_row, skip in ((owner, stand_in & home), (row, stand_in)):
        for dc in range(1, ncol):
            if dc != behind:
                greet_for(to_row, dc)

        @pl.when(jnp.logical_not(skip))
        def _():
            greet_for(to_row, behind)

    @pl.when(jnp.logical_not(home))
    def _():
        greet_for(owner, 0)

    def send(src, dst, send_sem, recv_sem, to_row, to_col):
        pltpu.make_async_remote_copy(
            src_ref=src, dst_ref=dst, send_sem=send_sem, recv_sem=recv_sem,
            device_id=(to_row, to_col), device_id_type=pl.DeviceIdType.MESH,
        ).start()

    def place(src, dst, send_sem, recv_sem, to_row, to_col, here):
        @pl.when(here)
        def _():
            pltpu.make_async_copy(src, dst, recv_sem).start()

        @pl.when(jnp.logical_not(here))
        def _():
            send(src, dst, send_sem, recv_sem, to_row, to_col)

    def to_peers(src, dst, send_sem, recv_sem):
        for dc in far_first(ncol)[:-1]:
            send(src, dst, send_sem, recv_sem, row, wrap(col + dc, ncol))

    def expect(ref, sem):
        pltpu.make_async_copy(ref, ref, sem).wait()

    def settle(ref, sem, here):
        count = ref.shape[1]

        @pl.when(jnp.logical_not(here))
        def _():
            expect(ref, sem)

        if count > 1:
            @pl.when(here)
            def _():
                expect(ref.at[:, pl.ds(0, count - 1)], sem)

    def spread_out(h, src, dst, send_sem, recv_sem):
        for dr in far_first(nrow)[:-1]:
            send(src, dst, send_sem, recv_sem, wrap(row + dr, nrow), row * split + h)

    def spread_here(h, src, dst, send_sem, recv_sem):
        to_col = row * split + h
        place(src, dst, send_sem, recv_sem, row, to_col, to_col == col)

    @pl.when(col == 0)
    def _():
        head.wait()
        for h in range(split):
            def turn(t, carry):
                at = pl.multiple_of(h * cols_local + t * LANES, LANES)
                block = first_ref[pl.ds(at, LANES), :].T
                for k in range(NB + 1):
                    pan_ref[k, h, pl.ds(t, 1), :] = block[k : k + 1, :]
                return carry

            lax.fori_loop(0, tiles, turn, 0)

    one = jnp.where(home, 1, 0)
    partners = split * nrow + ncol - 1 - one
    front_home = jnp.where((col - CHIPS_X) // split == row, 1, 0)
    proxied = partners - 1 + one - front_home - one
    kids = (planes - 1) * jnp.where(twice, 2, 1)
    first = jnp.where(core == 0, nrow, split * nrow)
    first = jnp.where(y == 0, split * nrow - one, first)
    count = jnp.where(stand_in, partners + proxied, partners)
    count = jnp.where(source, first, jnp.where(relay, kids, count))
    pl.semaphore_wait(barrier, count)

    @pl.when(stand_in)
    def _():
        pl.semaphore_signal(
            go_sem, inc=1, device_id=(row, col - CHIPS_X),
            device_id_type=pl.DeviceIdType.MESH,
        )

    def pan_span(i):
        return pl.ds(2 * i, min(2, NB + 1 - 2 * i))

    def send_pan(i):
        @pl.when(col == 0)
        def _():
            for spread in (spread_out, spread_here):
                for h in range(split):
                    spread(
                        h, pan_ref.at[pan_span(i), h], mypan_ref.at[pan_span(i)],
                        pan_send, pan_sem.at[i],
                    )

    head_span = pan_span(0)

    @pl.when(source & (y == 0))
    def _():
        for spread in (spread_out, spread_here):
            for h in range(split):
                spread(
                    h, pan_ref.at[head_span, h], mypan_ref.at[head_span],
                    head_send, pan_sem.at[0],
                )

    @pl.when(source & (y > 0))
    def _():
        for dr in far_first(nrow):
            for h in range(split):
                to_x = core * split + h
                moved = jnp.where(to_x == 0, 1, 0)
                send(
                    pan_ref.at[head_span, h], relay_ref.at[moved, y],
                    head_send, relay_sem.at[moved, y], wrap(row + dr, nrow), to_x + moved,
                )

    def hand_on(i):
        for plane in far_first(planes)[:-1]:
            piece = relay_ref.at[i, plane]
            expect(piece, relay_sem.at[i, plane])
            send(
                piece, mypan_ref.at[head_span], kid_send.at[i], pan_sem.at[0],
                row, plane * CHIPS_X + x - i,
            )

    @pl.when(relay)
    def _():
        hand_on(0)

    @pl.when(twice)
    def _():
        hand_on(1)

    @pl.when(front)
    def _():
        pl.semaphore_wait(go_sem, 1)

    def fold(acc, h, t, j):
        part_ref[j, h, t : t + 1, :] = jnp.sum(acc.T, axis=0, keepdims=True)

    def matvec(j, vector, act):
        pieces = [
            jnp.broadcast_to(vector[t : t + 1, :], (SUB, LANES)) for t in range(tiles)
        ]

        def product(t):
            accs = []
            for s in range(LANES // SUB):
                at = pl.ds(t * LANES + s * SUB, SUB)
                acc = a_ref[at, pl.ds(0, LANES)] * pieces[0]
                for p in range(1, tiles):
                    acc = acc + a_ref[at, pl.ds(p * LANES, LANES)] * pieces[p]
                accs.append(acc)
            return jnp.concatenate(accs, axis=0)

        for h in range(split):
            for t in range(tiles):
                fold(product(h * tiles + t), h, t, j)
            act(h)

    def own_rows(src, dst, send_sem, recv_sem):
        @pl.when(home)
        def _():
            to_peers(src, dst(slot), send_sem, recv_sem)
            pltpu.make_async_copy(src, dst(slot), recv_sem).start()

    def lay_out(ref, out, k):
        for h in range(split):
            for t in range(tiles):
                span = pl.ds((h * tiles + t) * LANES, LANES)
                out[k : k + 1, span] = ref[k, h, t : t + 1, :]

    def publish(src, ref, j, send_sem, recv_sem):
        for i in range(split):
            to_col = row * split + i
            here = jnp.logical_and(home, to_col == col)
            place(src, ref.at[j, slot], send_sem, recv_sem, owner, to_col, here)

    lane = lax.broadcasted_iota(jnp.int32, (1, LANES), 1)
    at_stat = lax.broadcasted_iota(jnp.int32, (STATS, LANES), 0) + STATS
    at_lane = lax.broadcasted_iota(jnp.int32, (STATS, LANES), 1)
    line_ids = lax.broadcasted_iota(jnp.int32, (tiles, LANES), 0) * LANES
    ids = line_ids + lax.broadcasted_iota(jnp.int32, (tiles, LANES), 1)
    ids = ids + col * cols_local
    hess_out[...] = jnp.zeros_like(hess_out)

    def send_stats(j, b):
        rows = [jnp.sum(vec_ref[k] * b, axis=0, keepdims=True) for k in range(j)]
        rows += [jnp.zeros((1, LANES), F32)] * (NB - j)
        rows.append(jnp.sum(b * b, axis=0, keepdims=True))
        rows += [jnp.zeros((1, LANES), F32)] * (STATS - NB - 1)
        sums = jnp.sum(jnp.concatenate(rows, axis=0), axis=1, keepdims=True)
        packed = jnp.where(at_lane == at_stat, sums, F32(0.0))
        packed = jnp.sum(packed, axis=0, keepdims=True)
        top = jnp.where(jnp.logical_and(col == 0, lane < STATS), b[0:1, :], packed)
        stat_ref[j] = top
        stats_ref[j, col] = top
        to_peers(stat_ref.at[j], stats_ref.at[j, col], stat_send, stat_sem.at[j])

    def total(ref, count):
        terms = [ref[i] for i in range(count)]
        while len(terms) > 1:
            terms = [x + y for x, y in zip(terms[::2], terms[1::2])]
        return terms[0]

    factor = [[None] * NB for _ in range(NB)]
    gram = [[None] * NB for _ in range(NB)]
    tops = []
    images = []
    for i in range(blocks):
        block_load(i).wait()
    expect(mypan_ref.at[pan_span(0)], pan_sem.at[0])
    b = mypan_ref[0]
    for j in range(NB):
        if j < last:
            def share(spread, h):
                spread(
                    h, part_ref.at[j, h], got_ref.at[j, col], part_send, part_sem.at[j]
                )

            matvec(j, b, functools.partial(share, spread_out))
            for h in range(split):
                share(spread_here, h)
            send_stats(j, b)
            if j > 0:
                publish(yvec_ref.at[j - 1], wy_ref, j - 1, y_send, y_sem)
            if j < NB // 2:
                send_pan(j + 1)
        else:
            send_stats(j, b)
            tail_ref[0] = b
            tail_ref[1] = yvec_ref[j - 1]
            matvec(j, b, lambda h: None)
            sums_ref[col] = part_ref[j]
            to_peers(part_ref.at[j], sums_ref.at[col], sum_send, sum_sem)
            own_rows(tail_ref, lambda at: ends_ref.at[at], tail_send, tail_sem)

        expect(stats_ref.at[j, pl.ds(0, ncol - 1)], stat_sem.at[j])
        stat = total(stats_ref.at[j], ncol)
        inner = [stat[:, STATS + k : STATS + k + 1] for k in range(j)]
        top = jnp.where(lane < STATS, stat, F32(0.0))
        weight = []
        for m in range(j):
            value = factor[0][m] * inner[0]
            for k in range(1, m + 1):
                value = value + factor[k][m] * inner[k]
            weight.append(value)
        for m in range(j):
            top = top - tops[m] * weight[m]
        above = jnp.where(lane <= j, top, F32(0.0))
        square = stat[:, STATS + NB : STATS + NB + 1]
        square = square - jnp.sum(above * above, axis=1, keepdims=True)
        norm = jnp.sqrt(square)
        alpha = top[:, j + 1 : j + 2]
        signed = jnp.where(alpha >= 0, norm, -norm)
        scale = 1.0 / jnp.sqrt(norm * (norm + jnp.abs(alpha)))
        u = b
        for m in range(j):
            u = u - vec_ref[m] * weight[m]
        u = jnp.where(ids > j, u, F32(0.0)) + jnp.where(ids == j + 1, signed, F32(0.0))
        u = u * scale
        vec_ref[j] = u
        if j < last:
            publish(vec_ref.at[j], refl_ref, j, v_send, v_sem)
        vtop = jnp.where(lane > j, top, F32(0.0))
        vtop = (vtop + jnp.where(lane == j + 1, signed, F32(0.0))) * scale
        couple = []
        for k in range(j):
            value = inner[k]
            for m in range(j):
                value = value - gram[k][m] * weight[m]
            fix = jnp.where(lane == j + 1, signed, F32(0.0)) - above
            value = value + jnp.sum(tops[k] * fix, axis=1, keepdims=True)
            couple.append(value * scale)
        for k in range(j):
            value = factor[k][k] * couple[k]
            for m in range(k + 1, j):
                value = value + factor[k][m] * couple[m]
            factor[k][j] = -value
            gram[k][j] = couple[k]
            gram[j][k] = couple[k]
        factor[j][j] = jnp.ones((1, 1), F32)
        gram[j][j] = jnp.full((1, 1), 2.0, F32)
        tops.append(vtop)
        hrow = jnp.where(lane == j + 1, -signed, above)
        hess_out[j : j + 1, 0:LANES] = jnp.where(row == 0, hrow, F32(0.0))
        if 0 < j <= NB // 2:
            expect(mypan_ref.at[pan_span(j)], pan_sem.at[j])
        if j < last:
            drop = jnp.zeros((tiles, LANES), F32)
            for k in range(j):
                drop = drop + images[k] * weight[k]
            for i in range(j + 1):
                drop = drop + mypan_ref[i] * top[:, i : i + 1]
            drop = (drop - mypan_ref[j + 1] * signed) * scale
            back = jnp.zeros((tiles, LANES), F32)
            for k in range(j):
                back = back + yvec_ref[k] * couple[k]
            rest = mypan_ref[j + 1]
            for k in range(j):
                rest = rest - yvec_ref[k] * tops[k][:, j + 1 : j + 2]
            pull = vtop[:, j + 1 : j + 2]
            rest = rest + (drop + back) * pull
            coef_ref[0] = jnp.broadcast_to(pull * scale, (tiles, LANES))
            coef_ref[1] = jnp.broadcast_to(scale, (tiles, LANES))
            coef_ref[2] = rest
            if 0 < j <= NB // 2 + 1:
                own_rows(
                    mypan_ref.at[pan_span(j - 1)],
                    lambda at: edges_ref.at[at, pan_span(j - 1)],
                    edge_send, edge_sem,
                )

            expect(got_ref.at[j], part_sem.at[j])
            image = total(got_ref.at[j], ncol)
            b = coef_ref[2] - image * coef_ref[0]
            image = image * coef_ref[1] - drop
            images.append(image)
            yvec_ref[j] = image - back

    mix = []
    for m in range(last):
        value = weight[m]
        for k in range(m + 1, last):
            value = value + gram[m][k] * weight[k]
        mix.append(value * scale + couple[m])
    expect(edges_ref, edge_sem)
    expect(wy_ref.at[pl.ds(0, last - 1)], y_sem)
    rest = []
    for h in range(split):
        value = edges_ref[h, NB] * signed
        for i in range(NB):
            value = value - edges_ref[h, i] * top[:, i : i + 1]
        value = value * scale
        for k in range(last - 1):
            value = value - wy_ref[k, h] * mix[k]
        rest.append(value)
    expect(refl_ref.at[pl.ds(0, last)], v_sem)
    expect(ends_ref, tail_sem)
    for h in range(split):
        at = line_ids + lane + (row * rows_local + h * cols_local)
        u = ends_ref[h, 0]
        for m in range(last):
            u = u - refl_ref[m, h] * weight[m]
        u = jnp.where(at > last, u, F32(0.0)) + jnp.where(at == NB, signed, F32(0.0))
        refl_ref[last, h] = u * scale
        wy_ref[last - 1, h] = ends_ref[h, 1]
        rest[h] = rest[h] - ends_ref[h, 1] * mix[last - 1]

    at_row = lax.broadcasted_iota(jnp.int32, (NB, NB), 0)
    at_col = lax.broadcasted_iota(jnp.int32, (NB, NB), 1)
    fac = jnp.zeros((NB, NB), F32)
    for k in range(NB):
        for m in range(k, NB):
            here = jnp.logical_and(at_row == k, at_col == m)
            fac = jnp.where(here, jnp.broadcast_to(factor[k][m], (NB, NB)), fac)
    fac_ref[...] = fac

    expect(stats_ref.at[:, pl.ds(0, ncol - 1)], stat_send)
    settle(got_ref.at[pl.ds(0, last)], part_send, home)
    settle(refl_ref.at[pl.ds(0, last)], v_send, home)
    settle(wy_ref.at[pl.ds(0, last - 1)], y_send, home)

    @pl.when(home)
    def _():
        expect(got_ref.at[pl.ds(0, NB + 1), pl.ds(0, ncol - 1)], edge_send)

    for i, sent in enumerate((relay, twice)):
        @pl.when(sent)
        def _():
            expect(relay_ref.at[i, pl.ds(1, planes - 1)], kid_send.at[i])

    @pl.when(source)
    def _():
        settle(got_ref.at[pl.ds(0, NB - 1)], pan_send, row == 0)
        settle(got_ref.at[pl.ds(0, 2)], head_send, row == 0)

    for k in range(NB):
        lay_out(refl_ref, refl_out, k)
    for k in range(last):
        lay_out(wy_ref, wy_out, k)
    others = sums_ref.at[pl.ds(0, ncol - 1)]
    expect(others, sum_sem)
    image = total(sums_ref, ncol)
    for h in range(split):
        wy_ref[last, h] = image[h] * scale + rest[h]
    lay_out(wy_ref, wy_out, last)
    expect(others, sum_send)

    @pl.when(home)
    def _():
        expect(others, tail_send)


def finish(*refs):
    count = len(refs) // 2
    sems = refs[-1]
    copies = [
        pltpu.make_async_copy(refs[i], refs[count + i], sems.at[i]) for i in range(count)
    ]
    for copy in copies:
        copy.start()
    for copy in copies:
        copy.wait()


def shards(nrow, ncol, matrix):
    rows_local, cols_local = matrix.shape
    tiles = cols_local // LANES
    split = rows_local // cols_local
    blocks = rows_local // BLOCK
    panel = pltpu.VMEM((NB, rows_local), F32)
    vmem = pl.BlockSpec(memory_space=pltpu.VMEM)
    dma = pltpu.SemaphoreType.DMA
    hess, refl, wy, fac = pl.pallas_call(
        functools.partial(kernel, nrow, ncol),
        out_shape=(panel, panel, panel, pltpu.VMEM((NB, NB), F32)),
        in_specs=[pl.BlockSpec(memory_space=pl.ANY)],
        out_specs=(vmem, vmem, vmem, vmem),
        scratch_shapes=[
            pltpu.VMEM((NB, split, tiles, LANES), F32),
            pltpu.VMEM((NB, split, tiles, LANES), F32),
            pltpu.VMEM((rows_local, cols_local), F32),
            pltpu.VMEM((rows_local, LANES), F32),
            pltpu.VMEM((NB + 1, split, tiles, LANES), F32),
            pltpu.VMEM((NB + 1, tiles, LANES), F32),
            pltpu.VMEM((NB, split, tiles, LANES), F32),
            pltpu.VMEM((NB + 1, ncol, tiles, LANES), F32),
            pltpu.VMEM((NB, 1, LANES), F32),
            pltpu.VMEM((NB, ncol, 1, LANES), F32),
            pltpu.VMEM((NB, tiles, LANES), F32),
            pltpu.VMEM((NB, tiles, LANES), F32),
            pltpu.VMEM((split, NB + 1, tiles, LANES), F32),
            pltpu.VMEM((2, tiles, LANES), F32),
            pltpu.VMEM((split, 2, tiles, LANES), F32),
            pltpu.VMEM((ncol, split, tiles, LANES), F32),
            pltpu.VMEM((3, tiles, LANES), F32),
            pltpu.VMEM((2, ncol // CHIPS_X, 2, tiles, LANES), F32),
            dma((blocks,)),
            dma(()),
            dma(()),
            dma((NB // 2 + 1,)),
            dma(()),
            dma((NB,)),
            dma(()),
            dma((NB,)),
            dma(()),
            dma(()),
            dma(()),
            dma(()),
            dma(()),
            dma(()),
            dma(()),
            dma(()),
            dma(()),
            dma(()),
            dma(()),
            dma((2, ncol // CHIPS_X)),
            dma((2,)),
            pltpu.SemaphoreType.REGULAR,
        ],
        compiler_params=pltpu.CompilerParams(
            collective_id=0, has_side_effects=True, vmem_limit_bytes=56 * 2**20
        ),
    )(matrix)
    made = [
        pltpu.with_memory_space_constraint(x, pltpu.VMEM) for x in (hess, refl, wy, fac)
    ]
    hess, refl, wy, fac = pl.pallas_call(
        finish,
        out_shape=[jax.ShapeDtypeStruct(x.shape, F32) for x in made],
        in_specs=[vmem] * 4,
        out_specs=[pl.BlockSpec(memory_space=pl.ANY)] * 4,
        scratch_shapes=[dma((4,))],
    )(*made)
    return hess.T, refl.T, wy.T, fac


def solution(mesh):
    nrow, ncol = mesh.shape["row"], mesh.shape["col"]
    return jax.shard_map(
        functools.partial(shards, nrow, ncol),
        mesh=mesh,
        in_specs=(P("row", "col"),),
        out_specs=(P("row", None), P("row", None), P("row", None), P()),
        check_vma=False,
    )
```

```python
import functools

import jax
import jax.numpy as jnp
from jax import lax
from jax.experimental import pallas as pl
from jax.experimental.pallas import tpu as pltpu
from jax.sharding import PartitionSpec as P

NB = 8
LANES = 128
SUB = 8
STATS = 16
BLOCK = 256
CORES = 2
CHIPS_X = 4
F32 = jnp.float32


def kernel(
    nrow, ncol, a_hbm, hess_out, refl_out, wy_out, fac_ref,
    refl_ref, wy_ref, a_ref, first_ref, pan_ref, mypan_ref, part_ref, got_ref, stat_ref, stats_ref,
    vec_ref, yvec_ref, edges_ref, tail_ref, ends_ref, sums_ref, coef_ref, relay_ref,
    load_sem, first_sem, pan_send, pan_sem, stat_send, stat_sem,
    part_send, part_sem, v_send, v_sem, y_send, y_sem,
    edge_send, edge_sem, tail_send, tail_sem, sum_send, sum_sem,
    head_send, relay_sem, kid_send, go_sem,
):
    rows_local, cols_local = a_hbm.shape
    tiles = cols_local // LANES
    split = rows_local // cols_local
    row, col = lax.axis_index("row"), lax.axis_index("col")
    blocks = rows_local // BLOCK
    owner = col // split
    slot = col - owner * split
    home = owner == row
    last = NB - 1
    planes = ncol // CHIPS_X
    y, z = row // CORES, col // CHIPS_X
    core, x = row - y * CORES, col - z * CHIPS_X
    front = z == 0
    source = col == 0
    relay = front & (col > 0)
    stand_in = z == 1
    twice = col == 1

    def wrap(value, bound):
        return jnp.where(value >= bound, value - bound, value)

    def far_first(count):
        return sorted(range(count), key=lambda d: -min(d, count - d))

    def block_load(i):
        span = pl.ds(i * BLOCK, BLOCK)
        return pltpu.make_async_copy(a_hbm.at[span], a_ref.at[span], load_sem.at[i])

    head = pltpu.make_async_copy(a_hbm.at[:, pl.ds(0, LANES)], first_ref, first_sem)

    @pl.when(col == 0)
    def _():
        head.start()

    for i in range(blocks):
        block_load(i).start(priority=1)

    barrier = pltpu.get_barrier_semaphore()

    def greet(to_row, to_col):
        pl.semaphore_signal(
            barrier, inc=1, device_id=(to_row, to_col),
            device_id_type=pl.DeviceIdType.MESH,
        )

    @pl.when(jnp.logical_not(front))
    def _():
        greet(row, jnp.where(x == 0, 1, x))

    @pl.when(front & jnp.logical_not(home & source))
    def _():
        greet(owner, 0)

    @pl.when(relay)
    def _():
        for plane in range(1, planes):
            greet(plane * CORES + owner, 0)

    def greet_for(to_row, dc):
        to_col = wrap(col + dc, ncol)
        greet(to_row, jnp.where(to_col < CHIPS_X, to_col + CHIPS_X, to_col))

    behind = ncol - CHIPS_X
    for to_row, skip in ((owner, stand_in & home), (row, stand_in)):
        for dc in range(1, ncol):
            if dc != behind:
                greet_for(to_row, dc)

        @pl.when(jnp.logical_not(skip))
        def _():
            greet_for(to_row, behind)

    @pl.when(jnp.logical_not(home))
    def _():
        greet_for(owner, 0)

    def send(src, dst, send_sem, recv_sem, to_row, to_col):
        pltpu.make_async_remote_copy(
            src_ref=src, dst_ref=dst, send_sem=send_sem, recv_sem=recv_sem,
            device_id=(to_row, to_col), device_id_type=pl.DeviceIdType.MESH,
        ).start()

    def place(src, dst, send_sem, recv_sem, to_row, to_col, here):
        @pl.when(here)
        def _():
            pltpu.make_async_copy(src, dst, recv_sem).start()

        @pl.when(jnp.logical_not(here))
        def _():
            send(src, dst, send_sem, recv_sem, to_row, to_col)

    def to_peers(src, dst, send_sem, recv_sem):
        for dc in far_first(ncol)[:-1]:
            send(src, dst, send_sem, recv_sem, row, wrap(col + dc, ncol))

    def expect(ref, sem):
        pltpu.make_async_copy(ref, ref, sem).wait()

    def settle(ref, sem, here):
        count = ref.shape[1]

        @pl.when(jnp.logical_not(here))
        def _():
            expect(ref, sem)

        if count > 1:
            @pl.when(here)
            def _():
                expect(ref.at[:, pl.ds(0, count - 1)], sem)

    def spread_out(h, src, dst, send_sem, recv_sem):
        for dr in far_first(nrow)[:-1]:
            send(src, dst, send_sem, recv_sem, wrap(row + dr, nrow), row * split + h)

    def spread_here(h, src, dst, send_sem, recv_sem):
        to_col = row * split + h
        place(src, dst, send_sem, recv_sem, row, to_col, to_col == col)

    @pl.when(col == 0)
    def _():
        head.wait()
        for h in range(split):
            def turn(t, carry):
                at = pl.multiple_of(h * cols_local + t * LANES, LANES)
                block = first_ref[pl.ds(at, LANES), :].T
                for k in range(NB + 1):
                    pan_ref[k, h, pl.ds(t, 1), :] = block[k : k + 1, :]
                return carry

            lax.fori_loop(0, tiles, turn, 0)

    one = jnp.where(home, 1, 0)
    partners = split * nrow + ncol - 1 - one
    front_home = jnp.where((col - CHIPS_X) // split == row, 1, 0)
    proxied = partners - 1 + one - front_home - one
    kids = (planes - 1) * jnp.where(twice, 2, 1)
    first = jnp.where(core == 0, nrow, split * nrow)
    first = jnp.where(y == 0, split * nrow - one, first)
    count = jnp.where(stand_in, partners + proxied, partners)
    count = jnp.where(source, first, jnp.where(relay, kids, count))
    pl.semaphore_wait(barrier, count)

    @pl.when(stand_in)
    def _():
        pl.semaphore_signal(
            go_sem, inc=1, device_id=(row, col - CHIPS_X),
            device_id_type=pl.DeviceIdType.MESH,
        )

    def pan_span(i):
        return pl.ds(2 * i, min(2, NB + 1 - 2 * i))

    def send_pan(i):
        @pl.when(col == 0)
        def _():
            for spread in (spread_out, spread_here):
                for h in range(split):
                    spread(
                        h, pan_ref.at[pan_span(i), h], mypan_ref.at[pan_span(i)],
                        pan_send, pan_sem.at[i],
                    )

    head_span = pan_span(0)

    @pl.when(source & (y == 0))
    def _():
        for spread in (spread_out, spread_here):
            for h in range(split):
                spread(
                    h, pan_ref.at[head_span, h], mypan_ref.at[head_span],
                    head_send, pan_sem.at[0],
                )

    @pl.when(source & (y > 0))
    def _():
        for dr in far_first(nrow):
            for h in range(split):
                to_x = core * split + h
                moved = jnp.where(to_x == 0, 1, 0)
                send(
                    pan_ref.at[head_span, h], relay_ref.at[moved, y],
                    head_send, relay_sem.at[moved, y], wrap(row + dr, nrow), to_x + moved,
                )

    def hand_on(i):
        for plane in far_first(planes)[:-1]:
            piece = relay_ref.at[i, plane]
            expect(piece, relay_sem.at[i, plane])
            send(
                piece, mypan_ref.at[head_span], kid_send.at[i], pan_sem.at[0],
                row, plane * CHIPS_X + x - i,
            )

    @pl.when(relay)
    def _():
        hand_on(0)

    @pl.when(twice)
    def _():
        hand_on(1)

    def fold(acc, h, t, j):
        part_ref[j, h, t : t + 1, :] = jnp.sum(acc.T, axis=0, keepdims=True)

    def matvec(j, vector, act):
        pieces = [
            jnp.broadcast_to(vector[t : t + 1, :], (SUB, LANES)) for t in range(tiles)
        ]

        def product(t):
            accs = []
            for s in range(LANES // SUB):
                at = pl.ds(t * LANES + s * SUB, SUB)
                acc = a_ref[at, pl.ds(0, LANES)] * pieces[0]
                for p in range(1, tiles):
                    acc = acc + a_ref[at, pl.ds(p * LANES, LANES)] * pieces[p]
                accs.append(acc)
            return jnp.concatenate(accs, axis=0)

        for h in range(split):
            for t in range(tiles):
                fold(product(h * tiles + t), h, t, j)
            act(h)

    def own_rows(src, dst, send_sem, recv_sem):
        @pl.when(home)
        def _():
            to_peers(src, dst(slot), send_sem, recv_sem)
            pltpu.make_async_copy(src, dst(slot), recv_sem).start()

    def lay_out(ref, out, k):
        for h in range(split):
            for t in range(tiles):
                span = pl.ds((h * tiles + t) * LANES, LANES)
                out[k : k + 1, span] = ref[k, h, t : t + 1, :]

    def publish(src, ref, j, send_sem, recv_sem):
        for i in range(split):
            to_col = row * split + i
            here = jnp.logical_and(home, to_col == col)
            place(src, ref.at[j, slot], send_sem, recv_sem, owner, to_col, here)

    lane = lax.broadcasted_iota(jnp.int32, (1, LANES), 1)
    at_stat = lax.broadcasted_iota(jnp.int32, (STATS, LANES), 0) + STATS
    at_lane = lax.broadcasted_iota(jnp.int32, (STATS, LANES), 1)
    line_ids = lax.broadcasted_iota(jnp.int32, (tiles, LANES), 0) * LANES
    ids = line_ids + lax.broadcasted_iota(jnp.int32, (tiles, LANES), 1)
    ids = ids + col * cols_local
    hess_out[...] = jnp.zeros_like(hess_out)

    def send_stats(j, b):
        rows = [jnp.sum(vec_ref[k] * b, axis=0, keepdims=True) for k in range(j)]
        rows += [jnp.zeros((1, LANES), F32)] * (NB - j)
        rows.append(jnp.sum(b * b, axis=0, keepdims=True))
        rows += [jnp.zeros((1, LANES), F32)] * (STATS - NB - 1)
        sums = jnp.sum(jnp.concatenate(rows, axis=0), axis=1, keepdims=True)
        packed = jnp.where(at_lane == at_stat, sums, F32(0.0))
        packed = jnp.sum(packed, axis=0, keepdims=True)
        top = jnp.where(jnp.logical_and(col == 0, lane < STATS), b[0:1, :], packed)
        stat_ref[j] = top
        stats_ref[j, col] = top
        to_peers(stat_ref.at[j], stats_ref.at[j, col], stat_send, stat_sem.at[j])

    def total(ref, count):
        terms = [ref[i] for i in range(count)]
        while len(terms) > 1:
            terms = [x + y for x, y in zip(terms[::2], terms[1::2])]
        return terms[0]

    factor = [[None] * NB for _ in range(NB)]
    gram = [[None] * NB for _ in range(NB)]
    tops = []
    images = []
    for i in range(blocks):
        block_load(i).wait()
    expect(mypan_ref.at[pan_span(0)], pan_sem.at[0])
    b = mypan_ref[0]
    for j in range(NB):
        if j < last:
            def share(spread, h):
                if j == 0 and h == 0 and spread is spread_out:
                    @pl.when(front)
                    def _():
                        pl.semaphore_wait(go_sem, 1)

                spread(
                    h, part_ref.at[j, h], got_ref.at[j, col], part_send, part_sem.at[j]
                )

            matvec(j, b, functools.partial(share, spread_out))
            for h in range(split):
                share(spread_here, h)
            send_stats(j, b)
            if j > 0:
                publish(yvec_ref.at[j - 1], wy_ref, j - 1, y_send, y_sem)
            if j < NB // 2:
                send_pan(j + 1)
        else:
            tail_ref[0] = b
            tail_ref[1] = yvec_ref[j - 1]
            matvec(j, b, lambda h: send_stats(j, b) if h == 0 else None)
            sums_ref[col] = part_ref[j]
            to_peers(part_ref.at[j], sums_ref.at[col], sum_send, sum_sem)
            own_rows(tail_ref, lambda at: ends_ref.at[at], tail_send, tail_sem)

        expect(stats_ref.at[j, pl.ds(0, ncol - 1)], stat_sem.at[j])
        stat = total(stats_ref.at[j], ncol)
        inner = [stat[:, STATS + k : STATS + k + 1] for k in range(j)]
        top = jnp.where(lane < STATS, stat, F32(0.0))
        weight = []
        for m in range(j):
            value = factor[0][m] * inner[0]
            for k in range(1, m + 1):
                value = value + factor[k][m] * inner[k]
            weight.append(value)
        for m in range(j):
            top = top - tops[m] * weight[m]
        above = jnp.where(lane <= j, top, F32(0.0))
        square = stat[:, STATS + NB : STATS + NB + 1]
        square = square - jnp.sum(above * above, axis=1, keepdims=True)
        norm = jnp.sqrt(square)
        alpha = top[:, j + 1 : j + 2]
        signed = jnp.where(alpha >= 0, norm, -norm)
        scale = 1.0 / jnp.sqrt(norm * (norm + jnp.abs(alpha)))
        u = b
        for m in range(j):
            u = u - vec_ref[m] * weight[m]
        u = jnp.where(ids > j, u, F32(0.0)) + jnp.where(ids == j + 1, signed, F32(0.0))
        u = u * scale
        vec_ref[j] = u
        if j < last:
            publish(vec_ref.at[j], refl_ref, j, v_send, v_sem)
        vtop = jnp.where(lane > j, top, F32(0.0))
        vtop = (vtop + jnp.where(lane == j + 1, signed, F32(0.0))) * scale
        couple = []
        for k in range(j):
            value = inner[k]
            for m in range(j):
                value = value - gram[k][m] * weight[m]
            fix = jnp.where(lane == j + 1, signed, F32(0.0)) - above
            value = value + jnp.sum(tops[k] * fix, axis=1, keepdims=True)
            couple.append(value * scale)
        for k in range(j):
            value = factor[k][k] * couple[k]
            for m in range(k + 1, j):
                value = value + factor[k][m] * couple[m]
            factor[k][j] = -value
            gram[k][j] = couple[k]
            gram[j][k] = couple[k]
        factor[j][j] = jnp.ones((1, 1), F32)
        gram[j][j] = jnp.full((1, 1), 2.0, F32)
        tops.append(vtop)
        hrow = jnp.where(lane == j + 1, -signed, above)
        hess_out[j : j + 1, 0:LANES] = jnp.where(row == 0, hrow, F32(0.0))
        if 0 < j <= NB // 2:
            expect(mypan_ref.at[pan_span(j)], pan_sem.at[j])
        if j < last:
            drop = jnp.zeros((tiles, LANES), F32)
            for k in range(j):
                drop = drop + images[k] * weight[k]
            for i in range(j + 1):
                drop = drop + mypan_ref[i] * top[:, i : i + 1]
            drop = (drop - mypan_ref[j + 1] * signed) * scale
            back = jnp.zeros((tiles, LANES), F32)
            for k in range(j):
                back = back + yvec_ref[k] * couple[k]
            rest = mypan_ref[j + 1]
            for k in range(j):
                rest = rest - yvec_ref[k] * tops[k][:, j + 1 : j + 2]
            pull = vtop[:, j + 1 : j + 2]
            rest = rest + (drop + back) * pull
            coef_ref[0] = jnp.broadcast_to(pull * scale, (tiles, LANES))
            coef_ref[1] = jnp.broadcast_to(scale, (tiles, LANES))
            coef_ref[2] = rest
            if 0 < j <= NB // 2 + 1:
                own_rows(
                    mypan_ref.at[pan_span(j - 1)],
                    lambda at: edges_ref.at[at, pan_span(j - 1)],
                    edge_send, edge_sem,
                )

            expect(got_ref.at[j], part_sem.at[j])
            image = total(got_ref.at[j], ncol)
            b = coef_ref[2] - image * coef_ref[0]
            image = image * coef_ref[1] - drop
            images.append(image)
            yvec_ref[j] = image - back

    mix = []
    for m in range(last):
        value = weight[m]
        for k in range(m + 1, last):
            value = value + gram[m][k] * weight[k]
        mix.append(value * scale + couple[m])
    expect(edges_ref, edge_sem)
    expect(wy_ref.at[pl.ds(0, last - 1)], y_sem)
    rest = []
    for h in range(split):
        value = edges_ref[h, NB] * signed
        for i in range(NB):
            value = value - edges_ref[h, i] * top[:, i : i + 1]
        value = value * scale
        for k in range(last - 1):
            value = value - wy_ref[k, h] * mix[k]
        rest.append(value)
    expect(refl_ref.at[pl.ds(0, last)], v_sem)
    expect(ends_ref, tail_sem)
    for h in range(split):
        at = line_ids + lane + (row * rows_local + h * cols_local)
        u = ends_ref[h, 0]
        for m in range(last):
            u = u - refl_ref[m, h] * weight[m]
        u = jnp.where(at > last, u, F32(0.0)) + jnp.where(at == NB, signed, F32(0.0))
        refl_ref[last, h] = u * scale
        wy_ref[last - 1, h] = ends_ref[h, 1]
        rest[h] = rest[h] - ends_ref[h, 1] * mix[last - 1]

    at_row = lax.broadcasted_iota(jnp.int32, (NB, NB), 0)
    at_col = lax.broadcasted_iota(jnp.int32, (NB, NB), 1)
    fac = jnp.zeros((NB, NB), F32)
    for k in range(NB):
        for m in range(k, NB):
            here = jnp.logical_and(at_row == k, at_col == m)
            fac = jnp.where(here, jnp.broadcast_to(factor[k][m], (NB, NB)), fac)
    fac_ref[...] = fac

    expect(stats_ref.at[:, pl.ds(0, ncol - 1)], stat_send)
    settle(got_ref.at[pl.ds(0, last)], part_send, home)
    settle(refl_ref.at[pl.ds(0, last)], v_send, home)
    settle(wy_ref.at[pl.ds(0, last - 1)], y_send, home)

    @pl.when(home)
    def _():
        expect(got_ref.at[pl.ds(0, NB + 1), pl.ds(0, ncol - 1)], edge_send)

    for i, sent in enumerate((relay, twice)):
        @pl.when(sent)
        def _():
            expect(relay_ref.at[i, pl.ds(1, planes - 1)], kid_send.at[i])

    @pl.when(source)
    def _():
        settle(got_ref.at[pl.ds(0, NB - 1)], pan_send, row == 0)
        settle(got_ref.at[pl.ds(0, 2)], head_send, row == 0)

    for k in range(NB):
        lay_out(refl_ref, refl_out, k)
    for k in range(last):
        lay_out(wy_ref, wy_out, k)
    others = sums_ref.at[pl.ds(0, ncol - 1)]
    expect(others, sum_sem)
    image = total(sums_ref, ncol)
    for h in range(split):
        wy_ref[last, h] = image[h] * scale + rest[h]
    lay_out(wy_ref, wy_out, last)
    expect(others, sum_send)

    @pl.when(home)
    def _():
        expect(others, tail_send)


def finish(*refs):
    count = len(refs) // 2
    sems = refs[-1]
    copies = [
        pltpu.make_async_copy(refs[i], refs[count + i], sems.at[i]) for i in range(count)
    ]
    for copy in copies:
        copy.start()
    for copy in copies:
        copy.wait()


def shards(nrow, ncol, matrix):
    rows_local, cols_local = matrix.shape
    tiles = cols_local // LANES
    split = rows_local // cols_local
    blocks = rows_local // BLOCK
    panel = pltpu.VMEM((NB, rows_local), F32)
    vmem = pl.BlockSpec(memory_space=pltpu.VMEM)
    dma = pltpu.SemaphoreType.DMA
    hess, refl, wy, fac = pl.pallas_call(
        functools.partial(kernel, nrow, ncol),
        out_shape=(panel, panel, panel, pltpu.VMEM((NB, NB), F32)),
        in_specs=[pl.BlockSpec(memory_space=pl.ANY)],
        out_specs=(vmem, vmem, vmem, vmem),
        scratch_shapes=[
            pltpu.VMEM((NB, split, tiles, LANES), F32),
            pltpu.VMEM((NB, split, tiles, LANES), F32),
            pltpu.VMEM((rows_local, cols_local), F32),
            pltpu.VMEM((rows_local, LANES), F32),
            pltpu.VMEM((NB + 1, split, tiles, LANES), F32),
            pltpu.VMEM((NB + 1, tiles, LANES), F32),
            pltpu.VMEM((NB, split, tiles, LANES), F32),
            pltpu.VMEM((NB + 1, ncol, tiles, LANES), F32),
            pltpu.VMEM((NB, 1, LANES), F32),
            pltpu.VMEM((NB, ncol, 1, LANES), F32),
            pltpu.VMEM((NB, tiles, LANES), F32),
            pltpu.VMEM((NB, tiles, LANES), F32),
            pltpu.VMEM((split, NB + 1, tiles, LANES), F32),
            pltpu.VMEM((2, tiles, LANES), F32),
            pltpu.VMEM((split, 2, tiles, LANES), F32),
            pltpu.VMEM((ncol, split, tiles, LANES), F32),
            pltpu.VMEM((3, tiles, LANES), F32),
            pltpu.VMEM((2, ncol // CHIPS_X, 2, tiles, LANES), F32),
            dma((blocks,)),
            dma(()),
            dma(()),
            dma((NB // 2 + 1,)),
            dma(()),
            dma((NB,)),
            dma(()),
            dma((NB,)),
            dma(()),
            dma(()),
            dma(()),
            dma(()),
            dma(()),
            dma(()),
            dma(()),
            dma(()),
            dma(()),
            dma(()),
            dma(()),
            dma((2, ncol // CHIPS_X)),
            dma((2,)),
            pltpu.SemaphoreType.REGULAR,
        ],
        compiler_params=pltpu.CompilerParams(
            collective_id=0, has_side_effects=True, vmem_limit_bytes=56 * 2**20
        ),
    )(matrix)
    made = [
        pltpu.with_memory_space_constraint(x, pltpu.VMEM) for x in (hess, refl, wy, fac)
    ]
    hess, refl, wy, fac = pl.pallas_call(
        finish,
        out_shape=[jax.ShapeDtypeStruct(x.shape, F32) for x in made],
        in_specs=[vmem] * 4,
        out_specs=[pl.BlockSpec(memory_space=pl.ANY)] * 4,
        scratch_shapes=[dma((4,))],
    )(*made)
    return hess.T, refl.T, wy.T, fac


def solution(mesh):
    nrow, ncol = mesh.shape["row"], mesh.shape["col"]
    return jax.shard_map(
        functools.partial(shards, nrow, ncol),
        mesh=mesh,
        in_specs=(P("row", "col"),),
        out_specs=(P("row", None), P("row", None), P("row", None), P()),
        check_vma=False,
    )
```
